32 devices in a mesh: dp: 8 (over z, y), rep: 4 (over x, core).
Axes of the slice: x: 2, y: 2, z: 4, core: 2. Of those that a mesh axis runs over, the one named last changes fastest.
Arguments:
- grads: bfloat16 [32, 4096, 512], P(('dp', 'rep')), may hold values from -1000 to 1000
- master: float32 [4096, 512], P('dp'), may hold values from -3 to 3
- first_moment: float32 [4096, 512], P('dp'), may hold values from -2 to 2
- second_moment: float32 [4096, 512], P('dp'), may hold values from 0.01 to 1
Outputs:
- weights: bfloat16 [4096, 512], replicated
- new_master: float32 [4096, 512], P('dp')
- new_first: float32 [4096, 512], P('dp')
- new_second: float32 [4096, 512], P('dp')
The draws below stay inside these ranges and needn't reach their ends.
All inputs are finite; a program needn't handle non-finite values.
Results may differ from the reference program's by a relative error of at most 0.001.
Values may be sent and summed in bfloat16 or wider, within the bound.
A program may use at most 64 MiB of HBM per device.

```python
import math
import jax
import jax.numpy as jnp
from jax import lax

D_WIN = 4096
STEP = 20
COLS = 512
SOURCES = 32
N_REP = 4


def draw_grads(key, part):
    keys = jax.random.split(jax.random.fold_in(key, 11), 3)
    position = jnp.arange(D_WIN, dtype=jnp.float32) / D_WIN
    replica = (jnp.arange(SOURCES, dtype=jnp.int32) % N_REP).astype(jnp.float32) / max(N_REP - 1, 1)
    row_scale = 10.0 ** jax.random.uniform(keys[0], (D_WIN,), jnp.float32) * 5.0 ** position
    col_scale = 10.0 ** jax.random.uniform(keys[1], (COLS,), jnp.float32)
    base = jax.random.normal(keys[2], (SOURCES, D_WIN, COLS), jnp.float32)
    base = base * (1.0 + 2.0 * replica)[:, None, None]
    scaled = base * row_scale[None, :, None] * col_scale[None, None, :]
    return jnp.clip(scaled, -1000.0, 1000.0).astype(jnp.bfloat16)


def block_levels(rng, shape, cuts, low, largest):
    level, own = 1.0, jax.random.fold_in(rng, 6)
    for axis_at, blocks in cuts:
        steps = jnp.exp(jax.random.uniform(jax.random.fold_in(own, axis_at), (blocks,), jnp.float32, low / len(cuts), largest / len(cuts)))
        level = level * jnp.repeat(steps, shape[axis_at] // blocks).reshape([-1 if axis == axis_at else 1 for axis in range(len(shape))])
    return level


def scatter_about(rng, dims, width, limit, cuts=(), held_as=jnp.bfloat16):
    values = width * jax.random.normal(rng, dims, jnp.float32)
    if cuts:
        values = values * block_levels(rng, dims, cuts, -0.22, 0.18)
    return jnp.clip(values, -limit, limit).astype(held_as)


def setup_inputs(seed: int = 0) -> dict:
    splits = jax.random.split(jax.random.key(seed), 5)
    return {
        "grads": draw_grads(jax.random.fold_in(splits[4], 71), 0),
        "master": scatter_about(splits[1], (D_WIN, COLS), 0.5, 3.0, ((0, 8),), jnp.float32),
        "first_moment": scatter_about(splits[2], (D_WIN, COLS), 0.3, 2.0, ((0, 8),), jnp.float32),
        "second_moment": jnp.clip(jnp.exp(math.log(1.0) - 4.6051702 * jax.random.uniform(splits[3], (D_WIN, COLS), jnp.float32) ** block_levels(splits[3], (D_WIN, COLS), ((0, 8),), -0.2, 0.2)), 0.01, 1.0),
    }


def adam_update(clipped, master, first_moment, second_moment):
    new_first = 0.9 * first_moment + 0.1 * clipped
    new_second = 0.95 * second_moment + 0.05 * clipped * clipped
    first_hat = new_first / (1.0 - 0.9 ** STEP)
    second_hat = new_second / (1.0 - 0.95 ** STEP)
    update = first_hat / (jnp.sqrt(second_hat) + 1e-08)
    new_master = master - 0.01 * (update + 0.1 * master)
    return (new_master, new_first, new_second)

def reference(grads, master, first_moment, second_moment):

    def accumulate(index, total):
        piece = lax.dynamic_index_in_dim(grads, index, 0, keepdims=False)
        return total + piece.astype(jnp.float32)
    total = lax.fori_loop(0, SOURCES, accumulate, jnp.zeros((D_WIN, COLS), jnp.float32))
    norm = jnp.sqrt(jnp.sum(total * total))
    threshold = 4.0 * math.sqrt(D_WIN * COLS)
    factor = jnp.minimum(1.0, threshold / (norm + 1e-06))
    new_master, new_first, new_second = adam_update(factor * total, master, first_moment, second_moment)
    return (new_master.astype(jnp.bfloat16), new_master, new_first, new_second)
```

```python
import functools
import math

import jax
import jax.numpy as jnp
from jax import lax
from jax.experimental import pallas as pl
from jax.experimental.pallas import tpu as pltpu
from jax.sharding import PartitionSpec as P

STEP = 20
MESH = pl.DeviceIdType.MESH
F32 = jnp.float32
PIECES, TRAIL = 2, (2, 4)
W_PIECES, W_TRAIL = 2, (2, 3)
VMEM_BYTES = 63 * 1024 * 1024
TOP = 2.0**14


def adam_update(clipped, master, first_moment, second_moment):
    new_first = 0.9 * first_moment + 0.1 * clipped
    new_second = 0.95 * second_moment + 0.05 * clipped * clipped
    first_hat = new_first / (1.0 - 0.9**STEP)
    second_hat = new_second / (1.0 - 0.95**STEP)
    update = first_hat / (jnp.sqrt(second_hat) + 1e-08)
    new_master = master - 0.01 * (update + 0.1 * master)
    return (new_master, new_first, new_second)


def clip_factor(squares, entries):
    threshold = 4.0 * math.sqrt(entries)
    return jnp.minimum(1.0, threshold / (jnp.sqrt(squares) + 1e-06))


def encode(value, scale):
    u = value * scale
    u2 = u * u
    u4 = u2 * u2
    return (u4 * u4 * u).astype(jnp.bfloat16)


def decode(coded, scale):
    w = coded.astype(F32)
    size = jnp.exp(jnp.log(jnp.abs(w)) * (1.0 / 9.0)) * scale
    return jnp.where(w < 0, -size, size)


def kernel(
    Z, R, entries,
    g, m_in, f_in, s_in,
    W, M, F, Q,
    L, swapped, S, EA, EB, E2, E3, RA, RB, R2, R3, V, N, B,
    load_sem, state_sem,
    g_sem, a1_sem, b1_sem, a2_sem, b2_sem, z_sem, n_sem, m_sem, v_sem,
    gz_sem, ga_sem, gb_sem, ha_sem, hb_sem, gc_sem,
):
    D = 2 * Z
    n = D * R
    d, r = lax.axis_index("dp"), lax.axis_index("rep")
    z, y = d // 2, d % 2
    x, c = r // 2, r % 2
    C, G = PIECES * Z, W_PIECES * Z
    to_x = (d, (1 - x) * 2 + c)
    to_y = (z * 2 + 1 - y, r)
    to_c = (d, x * 2 + 1 - c)

    def to_z(other):
        return (other * 2 + y, r)

    def push(src, dst, sems, index, device):
        return pltpu.make_async_remote_copy(
            src_ref=src, dst_ref=dst, send_sem=sems.at[(0,) + index], recv_sem=sems.at[(1,) + index],
            device_id=device, device_id_type=MESH,
        )

    def peer(k, sign):
        zz = (z + Z + sign * (k // 8)) % Z
        return zz, (y + k // 4) % 2, (x + k // 2) % 2, (c + k) % 2

    def to_peer(ref, sems, k):
        zz, yy, xx, cc = peer(k, 1)
        return push(ref.at[z, y, x, c], ref.at[z, y, x, c], sems, (k,), (zz * 2 + yy, xx * 2 + cc))

    def from_peer(ref, sems, k):
        zz, yy, xx, cc = peer(k, -1)
        return push(ref.at[zz, yy, xx, cc], ref.at[zz, yy, xx, cc], sems, (k,), (zz * 2 + yy, xx * 2 + cc))

    def dest(k):
        return (z + 1 + k) % Z

    def cols(q):
        width = g.shape[-1] // PIECES
        return pl.ds(pl.multiple_of((q % PIECES) * width, width), width)

    def w_cols(q):
        width = g.shape[-1] // W_PIECES
        return pl.ds(pl.multiple_of((q % W_PIECES) * width, width), width)

    barrier = pltpu.get_barrier_semaphore()

    @pl.loop(1, n)
    def _(k):
        zz, yy, xx, cc = peer(k, 1)
        pl.semaphore_signal(barrier, inc=1, device_id=(zz * 2 + yy, xx * 2 + cc), device_id_type=MESH)

    def load(k):
        return pltpu.make_async_copy(
            g.at[dest(k // PIECES), :, :, :, :, :, cols(k)], L.at[k // PIECES, :, :, :, :, :, cols(k)], load_sem.at[k]
        )

    @pl.loop(0, C)
    def _(k):
        load(k).start()

    states = [
        pltpu.make_async_copy(a, b, state_sem.at[i])
        for i, (a, b) in enumerate([(m_in, M), (f_in, F), (s_in, Q)])
    ]
    for copy in states:
        copy.start()

    B[z, y, x, c] = jnp.zeros((1, 128), F32)

    @pl.loop(0, C)
    def _(k):
        load(k).wait()
        size = jnp.abs(L[k // PIECES, :, :, :, :, :, cols(k)].astype(F32))
        lanes = jnp.max(size.reshape(-1, size.shape[-1]), axis=0, keepdims=True)
        best = B[z, y, x, c]
        for i in range(0, size.shape[-1], 128):
            best = jnp.maximum(best, lanes[:, i : i + 128])
        B[z, y, x, c] = best

    pl.semaphore_wait(barrier, n - 1)
    to_peer(B, m_sem, 1).start()

    def swap(k):
        return push(
            L.at[k // PIECES, :, 1 - c, :, :, :, cols(k)], swapped.at[k // PIECES, :, :, :, :, cols(k)],
            g_sem, (k,), to_c,
        )

    @pl.loop(0, C)
    def _(k):
        swap(k).start()

    @pl.loop(2, n)
    def _(k):
        to_peer(B, m_sem, k).start()

    def bound(rows):
        lanes = jnp.sum(rows.reshape(-1, 128), axis=0, keepdims=True)
        return jnp.maximum(jnp.max(lanes), 1e-30)

    def first_a(k):
        i, p = k // PIECES, cols(k)
        return push(EA.at[i, :, :, p], RA.at[i, :, :, p], a1_sem, (k,), to_x)

    def first_b(k):
        i, p = k // PIECES, cols(k)
        return push(EB.at[i, :, :, p], RB.at[i, :, :, p], b1_sem, (k,), to_y)

    def second_a(k):
        i, p = k // PIECES, cols(k)
        return push(E2.at[i, 0, :, p], R2.at[i, 0, :, p], a2_sem, (k,), to_y)

    def second_b(k):
        i, p = k // PIECES, cols(k)
        return push(E2.at[i, 1, :, p], R2.at[i, 1, :, p], b2_sem, (k,), to_x)

    def along_z(k):
        i, p = k // PIECES, cols(k)
        return push(E3.at[i, :, :, p], R3.at[i, :, :, p], z_sem, (k,), to_z(dest(i)))

    from_peer(B, m_sem, 1).wait_recv()
    own_bound = bound(B[z, y, x])
    own_scale = TOP / own_bound

    def stage1(k):
        i, p = k // PIECES, cols(k)
        swap(k).wait_recv()

        def pair(yy, xx, h):
            return L[i, yy, c, xx, h, :, p].astype(F32) + swapped[i, yy, xx, h, :, p].astype(F32)

        for yy in range(2):
            EA[i, yy, :, p] = encode(pair(yy, 1 - x, 0), own_scale)
        first_a(k).start()
        for xx in range(2):
            EB[i, xx, :, p] = encode(pair(1 - y, xx, 1), own_scale)
        first_b(k).start()
        for j in range(2):
            S[i, j, x, 0, :, p] = pair(j, x, 0)
            S[i, y, j, 1, :, p] = pair(y, j, 1)

    @pl.loop(0, TRAIL[0])
    def _(step):
        stage1(step)

    @pl.loop(2, n)
    def _(k):
        from_peer(B, m_sem, k).wait_recv()

    x_back = bound(B[z, y, 1 - x]) / TOP
    y_back = bound(B[z, 1 - y, x]) / TOP
    plane_bound = bound(B[z])
    plane_scale, plane_back = TOP / plane_bound, plane_bound / TOP
    whole_bound = bound(B[...])
    whole_scale, whole_back = TOP / whole_bound, whole_bound / TOP

    @pl.loop(TRAIL[0], C + TRAIL[1])
    def _(step):
        @pl.when(step < C)
        def _():
            stage1(step)

        @pl.when(step < C + TRAIL[0])
        def _():
            k = step - TRAIL[0]
            i, p = k // PIECES, cols(k)
            first_a(k).wait_recv()
            E2[i, 0, :, p] = encode(S[i, 1 - y, x, 0, :, p] + decode(RA[i, 1 - y, :, p], x_back), plane_scale)
            second_a(k).start()
            first_b(k).wait_recv()
            E2[i, 1, :, p] = encode(S[i, y, 1 - x, 1, :, p] + decode(RB[i, 1 - x, :, p], y_back), plane_scale)
            second_b(k).start()
            S[i, y, x, 0, :, p] = S[i, y, x, 0, :, p] + decode(RA[i, y, :, p], x_back)
            S[i, y, x, 1, :, p] = S[i, y, x, 1, :, p] + decode(RB[i, x, :, p], y_back)

        @pl.when(step >= TRAIL[1])
        def _():
            k = step - TRAIL[1]
            i, p = k // PIECES, cols(k)
            second_a(k).wait_recv()
            second_b(k).wait_recv()
            both = S[i, y, x, :, :, p] + decode(R2[i, :, :, p], plane_back)

            @pl.when(k < C - PIECES)
            def _():
                E3[i, :, :, p] = encode(both, whole_scale)
                along_z(k).start()

            @pl.when(k >= C - PIECES)
            def _():
                S[i, y, x, :, :, p] = both

    @pl.loop(0, C - PIECES)
    def _(k):
        i, p = k // PIECES, cols(k)
        along_z(k).wait_recv()
        S[Z - 1, y, x, :, :, p] = S[Z - 1, y, x, :, :, p] + decode(R3[i, :, :, p], whole_back)

    total = S[Z - 1, y, x]
    V[c, x] = total
    lanes = jnp.sum((total * total).reshape(-1, total.shape[-1]), axis=0, keepdims=True)
    N[z, y, x, c] = sum(lanes[:, i : i + 128] for i in range(0, total.shape[-1], 128))

    @pl.loop(1, n)
    def _(k):
        to_peer(N, n_sem, n - k).start()

    v_x = push(V.at[c, x], V.at[c, x], v_sem, (0,), to_x)
    v_c = push(V.at[c, x], V.at[c, x], v_sem, (1,), to_c)
    v_xc = push(V.at[c, 1 - x], V.at[c, 1 - x], v_sem, (2,), to_c)
    got_x = push(V.at[c, 1 - x], V.at[c, 1 - x], v_sem, (0,), to_x)
    got_c = push(V.at[1 - c, x], V.at[1 - c, x], v_sem, (1,), to_c)
    got_xc = push(V.at[1 - c, 1 - x], V.at[1 - c, 1 - x], v_sem, (2,), to_c)
    v_x.start()
    v_c.start()

    for copy in states:
        copy.wait()

    @pl.loop(1, n)
    def _(k):
        from_peer(N, n_sem, k).wait_recv()

    factor = clip_factor(jnp.sum(N[...]), entries)

    def update(cc, xx):
        new_master, new_first, new_second = adam_update(factor * V[cc, xx], M[cc, xx], F[cc, xx], Q[cc, xx])
        M[cc, xx] = new_master
        F[cc, xx] = new_first
        Q[cc, xx] = new_second
        W[z, y, cc, xx] = new_master.astype(jnp.bfloat16)

    update(c, x)

    def source(b):
        return (z + Z - b // W_PIECES) % Z

    def gather_z(j):
        block = W.at[z, y, c, x, :, :, w_cols(j)]
        return push(block, block, gz_sem, (j,), to_z(dest(j // W_PIECES)))

    def got_z(j):
        block = W.at[source(j + W_PIECES), y, c, x, :, :, w_cols(j)]
        return push(block, block, gz_sem, (j,), to_z(dest(j // W_PIECES)))

    def same(ref, sems, b, device):
        return push(ref, ref, sems, (b,), device)

    def own_a(b, yy):
        return same(W.at[z, yy, c, x, :, :, w_cols(b)], ga_sem, b, to_y)

    def own_h(b, xx):
        return same(W.at[z, 1 - y, c, xx, :, :, w_cols(b)], ha_sem, b, to_x)

    def own_c(b, cc):
        return same(W.at[z, 1 - y, cc, :, :, :, w_cols(b)], gc_sem, b, to_c)

    def ga(b, yy):
        return same(W.at[source(b), yy, c, x, 0, :, w_cols(b)], ga_sem, b, to_y)

    def gb(b, xx):
        return same(W.at[source(b), y, c, xx, 1, :, w_cols(b)], gb_sem, b, to_x)

    def ha(b, xx):
        return same(W.at[source(b), :, c, xx, 0, :, w_cols(b)], ha_sem, b, to_x)

    def hb(b, yy):
        return same(W.at[source(b), yy, c, :, 1, :, w_cols(b)], hb_sem, b, to_y)

    def gc(b, cc):
        return same(W.at[source(b), :, cc, :, :, :, w_cols(b)], gc_sem, b, to_c)

    @pl.loop(0, W_PIECES)
    def _(b):
        own_a(b, y).start()

    @pl.loop(0, G - W_PIECES)
    def _(j):
        gather_z(j).start()

    got_x.wait_recv()
    v_xc.start()
    update(c, 1 - x)
    got_c.wait_recv()
    update(1 - c, x)

    @pl.loop(0, W_PIECES)
    def _(b):
        own_a(b, 1 - y).wait_recv()
        own_h(b, x).start()

    @pl.loop(W_PIECES, G + W_TRAIL[1])
    def _(step):
        @pl.when((step >= W_PIECES + W_TRAIL[0]) & (step < G + W_TRAIL[0]))
        def _():
            b = step - W_TRAIL[0]
            ga(b, 1 - y).wait_recv()
            ha(b, x).start()
            gb(b, 1 - x).wait_recv()
            hb(b, y).start()

        @pl.when(step < G)
        def _():
            b = step
            got_z(b - W_PIECES).wait_recv()
            ga(b, y).start()
            gb(b, x).start()

        @pl.when(step == W_PIECES)
        def _():
            got_xc.wait_recv()
            update(1 - c, 1 - x)

            @pl.loop(0, W_PIECES)
            def _(b):
                own_h(b, 1 - x).wait_recv()
                own_c(b, c).start()

        @pl.when(step >= W_PIECES + W_TRAIL[1])
        def _():
            b = step - W_TRAIL[1]
            ha(b, 1 - x).wait_recv()
            hb(b, 1 - y).wait_recv()
            gc(b, c).start()

    @pl.loop(0, W_PIECES)
    def _(b):
        own_c(b, 1 - c).wait_recv()

    @pl.loop(W_PIECES, G)
    def _(b):
        gc(b, 1 - c).wait_recv()

    v_x.wait_send()
    v_c.wait_send()
    v_xc.wait_send()

    @pl.loop(1, n)
    def _(k):
        to_peer(B, m_sem, k).wait_send()
        to_peer(N, n_sem, k).wait_send()

    @pl.loop(0, C)
    def _(k):
        swap(k).wait_send()
        first_a(k).wait_send()
        first_b(k).wait_send()
        second_a(k).wait_send()
        second_b(k).wait_send()

    @pl.loop(0, C - PIECES)
    def _(k):
        along_z(k).wait_send()

    @pl.loop(0, W_PIECES)
    def _(b):
        own_a(b, y).wait_send()
        own_h(b, x).wait_send()
        own_c(b, c).wait_send()

    @pl.loop(W_PIECES, G)
    def _(b):
        ga(b, y).wait_send()
        gb(b, x).wait_send()
        ha(b, x).wait_send()
        hb(b, y).wait_send()
        gc(b, c).wait_send()

    @pl.loop(0, G - W_PIECES)
    def _(j):
        gather_z(j).wait_send()


def write_out(*refs):
    srcs, dsts, sems = refs[:4], refs[4:8], refs[8]
    copies = [pltpu.make_async_copy(a, b, sems.at[i]) for i, (a, b) in enumerate(zip(srcs, dsts))]
    for copy in copies:
        copy.start()
    for copy in copies:
        copy.wait()


def body(D, R, grads, master, first_moment, second_moment):
    rows, cols = grads.shape[1:]
    Z, n = D // 2, D * R
    t = rows // (D * R * 2)
    hbm = pl.BlockSpec(memory_space=pltpu.HBM)
    vmem = pl.BlockSpec(memory_space=pltpu.VMEM)
    bf16 = jnp.bfloat16
    part = (2, 2, 2, t, cols)
    dma = pltpu.SemaphoreType.DMA
    shapes = [((Z, 2) + part, bf16)] + [(part, F32)] * 3
    held_bytes = sum(math.prod(dims) * jnp.dtype(kind).itemsize for dims, kind in shapes)
    held = pl.pallas_call(
        functools.partial(kernel, Z, R, rows * cols),
        out_shape=[pltpu.VMEM(*shape) for shape in shapes],
        in_specs=[hbm] * 4,
        out_specs=[vmem] * 4,
        scratch_shapes=[
            pltpu.VMEM((Z, 2) + part, bf16),
            pltpu.VMEM((Z,) + part, bf16),
            pltpu.VMEM((Z,) + part, F32),
            pltpu.VMEM((Z, 2, t, cols), bf16),
            pltpu.VMEM((Z, 2, t, cols), bf16),
            pltpu.VMEM((Z, 2, t, cols), bf16),
            pltpu.VMEM((Z - 1, 2, t, cols), bf16),
            pltpu.VMEM((Z, 2, t, cols), bf16),
            pltpu.VMEM((Z, 2, t, cols), bf16),
            pltpu.VMEM((Z, 2, t, cols), bf16),
            pltpu.VMEM((Z - 1, 2, t, cols), bf16),
            pltpu.VMEM(part, F32),
            pltpu.VMEM((Z, 2, 2, 2, 1, 128), F32),
            pltpu.VMEM((Z, 2, 2, 2, 1, 128), F32),
            dma((PIECES * Z,)), dma((3,)),
            dma((2, PIECES * Z)), dma((2, PIECES * Z)), dma((2, PIECES * Z)),
            dma((2, PIECES * Z)), dma((2, PIECES * Z)), dma((2, PIECES * Z)),
            dma((2, n)), dma((2, n)), dma((2, 3)),
            dma((2, W_PIECES * Z)), dma((2, W_PIECES * Z)), dma((2, W_PIECES * Z)),
            dma((2, W_PIECES * Z)), dma((2, W_PIECES * Z)), dma((2, W_PIECES * Z)),
        ],
        compiler_params=pltpu.CompilerParams(
            collective_id=0, has_side_effects=True, vmem_limit_bytes=VMEM_BYTES - held_bytes
        ),
    )(
        grads.reshape((Z, 2) + part),
        master.reshape(part), first_moment.reshape(part), second_moment.reshape(part),
    )
    outs = pl.pallas_call(
        write_out,
        out_shape=[jax.ShapeDtypeStruct(*shape) for shape in shapes],
        in_specs=[vmem] * 4,
        out_specs=[hbm] * 4,
        scratch_shapes=[dma((4,))],
        compiler_params=pltpu.CompilerParams(vmem_limit_bytes=1024 * 1024),
    )(*held)
    weights, new_master, new_first, new_second = outs
    block = (rows // D, cols)
    return (weights.reshape(rows, cols), new_master.reshape(block), new_first.reshape(block), new_second.reshape(block))


def solution(mesh):
    D, R = mesh.shape["dp"], mesh.shape["rep"]
    assert R == 4 and D % 2 == 0
    in_specs = (P(("dp", "rep"), None, None), P("dp", None), P("dp", None), P("dp", None))
    out_specs = (P(), P("dp", None), P("dp", None), P("dp", None))
    return jax.shard_map(
        functools.partial(body, D, R), mesh=mesh, in_specs=in_specs, out_specs=out_specs, check_vma=False
    )
```

```python
import functools
import math

import jax
import jax.numpy as jnp
from jax import lax
from jax.experimental import pallas as pl
from jax.experimental.pallas import tpu as pltpu
from jax.sharding import PartitionSpec as P

STEP = 20
MESH = pl.DeviceIdType.MESH
F32 = jnp.float32
PIECES, TRAIL = 2, (2, 4)
W_PIECES, W_TRAIL = 2, (2, 3)
VMEM_BYTES = 63 * 1024 * 1024
TOP = 2.0**14
OWN, CORE, CHIP, FROM_X, FROM_Y, PAIR, PAIR_Y, PLANE, BELOW, UP, ABOVE, DOWN = range(12)


def adam_update(clipped, master, first_moment, second_moment):
    new_first = 0.9 * first_moment + 0.1 * clipped
    new_second = 0.95 * second_moment + 0.05 * clipped * clipped
    first_hat = new_first / (1.0 - 0.9**STEP)
    second_hat = new_second / (1.0 - 0.95**STEP)
    update = first_hat / (jnp.sqrt(second_hat) + 1e-08)
    new_master = master - 0.01 * (update + 0.1 * master)
    return (new_master, new_first, new_second)


def clip_factor(squares, entries):
    threshold = 4.0 * math.sqrt(entries)
    return jnp.minimum(1.0, threshold / (jnp.sqrt(squares) + 1e-06))


def encode(value, scale):
    u = value * scale
    u2 = u * u
    u4 = u2 * u2
    return (u4 * u4 * u).astype(jnp.bfloat16)


def decode(coded, scale):
    w = coded.astype(F32)
    size = jnp.exp(jnp.log(jnp.abs(w)) * (1.0 / 9.0)) * scale
    return jnp.where(w < 0, -size, size)


def kernel(
    Z, R, entries,
    g, m_in, f_in, s_in,
    W, M, F, Q,
    L, swapped, S, EA, EB, E2, E3, RA, RB, R2, RU, RD, V, N, B,
    load_sem, state_sem,
    g_sem, a1_sem, b1_sem, a2_sem, b2_sem, zu_sem, zd_sem, n_sem, m_sem, v_sem,
    gu_sem, gd_sem, ga_sem, gb_sem, ha_sem, hb_sem, gc_sem,
):
    D = 2 * Z
    n = D * R
    d, r = lax.axis_index("dp"), lax.axis_index("rep")
    z, y = d // 2, d % 2
    x, c = r // 2, r % 2
    C, G = PIECES * Z, W_PIECES * Z
    to_x = (d, (1 - x) * 2 + c)
    to_y = (z * 2 + 1 - y, r)
    to_c = (d, x * 2 + 1 - c)

    def to_z(other):
        return (other * 2 + y, r)

    def push(src, dst, sems, index, device):
        return pltpu.make_async_remote_copy(
            src_ref=src, dst_ref=dst, send_sem=sems.at[(0,) + index], recv_sem=sems.at[(1,) + index],
            device_id=device, device_id_type=MESH,
        )

    def peer(k, sign):
        zz = (z + Z + sign * (k // 8)) % Z
        return zz, (y + k // 4) % 2, (x + k // 2) % 2, (c + k) % 2

    def to_peer(ref, sems, k):
        zz, yy, xx, cc = peer(k, 1)
        return push(ref.at[z, y, x, c], ref.at[z, y, x, c], sems, (k,), (zz * 2 + yy, xx * 2 + cc))

    def from_peer(ref, sems, k):
        zz, yy, xx, cc = peer(k, -1)
        return push(ref.at[zz, yy, xx, cc], ref.at[zz, yy, xx, cc], sems, (k,), (zz * 2 + yy, xx * 2 + cc))

    below, above = z, Z - 1 - z
    near = jnp.minimum(below, above)

    def nth(j):
        paired = jnp.where(j % 2 == 1, z + (j + 1) // 2, z - (j + 1) // 2)
        single = jnp.where(below < above, z + j - near, z - j + near)
        return jnp.where(j <= 2 * near, paired, single)

    def dest(k):
        return nth(Z - 1 - k)

    def cols(q):
        width = g.shape[-1] // PIECES
        return pl.ds(pl.multiple_of((q % PIECES) * width, width), width)

    def w_cols(q):
        width = g.shape[-1] // W_PIECES
        return pl.ds(pl.multiple_of((q % W_PIECES) * width, width), width)

    B[...] = jnp.zeros(B.shape, F32)
    barrier = pltpu.get_barrier_semaphore()

    for device in (to_c, to_x, to_y):
        pl.semaphore_signal(barrier, inc=1, device_id=device, device_id_type=MESH)

    @pl.when(below > 0)
    def _():
        pl.semaphore_signal(barrier, inc=1, device_id=to_z(z - 1), device_id_type=MESH)

    @pl.when(above > 0)
    def _():
        pl.semaphore_signal(barrier, inc=1, device_id=to_z(z + 1), device_id_type=MESH)

    def load(k):
        return pltpu.make_async_copy(
            g.at[dest(k // PIECES), :, :, :, :, :, cols(k)], L.at[k // PIECES, :, :, :, :, :, cols(k)], load_sem.at[k]
        )

    @pl.loop(0, C)
    def _(k):
        load(k).start()

    states = [
        pltpu.make_async_copy(a, b, state_sem.at[i])
        for i, (a, b) in enumerate([(m_in, M), (f_in, F), (s_in, Q)])
    ]
    for copy in states:
        copy.start()

    @pl.loop(0, C)
    def _(k):
        load(k).wait()
        size = jnp.abs(L[k // PIECES, :, :, :, :, :, cols(k)].astype(F32))
        lanes = jnp.max(size.reshape(-1, size.shape[-1]), axis=0, keepdims=True)
        best = B[OWN]
        for i in range(0, size.shape[-1], 128):
            best = jnp.maximum(best, lanes[:, i : i + 128])
        B[OWN] = best

    pl.semaphore_wait(barrier, 3 + jnp.minimum(below, 1) + jnp.minimum(above, 1))

    def row(source, target, device):
        return push(B.at[source], B.at[target], m_sem, (target,), device)

    to_core = row(OWN, CORE, to_c)
    chip_x, chip_y = row(CHIP, FROM_X, to_x), row(CHIP, FROM_Y, to_y)
    pair_y = row(PAIR, PAIR_Y, to_y)
    row_up, row_down = row(UP, BELOW, to_z(z + 1)), row(DOWN, ABOVE, to_z(z - 1))

    def swap(k):
        return push(
            L.at[k // PIECES, :, 1 - c, :, :, :, cols(k)], swapped.at[k // PIECES, :, :, :, :, cols(k)],
            g_sem, (k,), to_c,
        )

    @pl.loop(0, C)
    def _(k):
        swap(k).start()

    to_core.start()

    def bound(index):
        return jnp.maximum(jnp.max(B[index]), 1e-30)

    def first_a(k):
        i, p = k // PIECES, cols(k)
        return push(EA.at[i, :, :, p], RA.at[i, :, :, p], a1_sem, (k,), to_x)

    def first_b(k):
        i, p = k // PIECES, cols(k)
        return push(EB.at[i, :, :, p], RB.at[i, :, :, p], b1_sem, (k,), to_y)

    def second_a(k):
        i, p = k // PIECES, cols(k)
        return push(E2.at[i, 0, :, p], R2.at[i, 0, :, p], a2_sem, (k,), to_y)

    def second_b(k):
        i, p = k // PIECES, cols(k)
        return push(E2.at[i, 1, :, p], R2.at[i, 1, :, p], b2_sem, (k,), to_x)

    def z_up(k):
        i, p = k // PIECES, cols(k)
        q = dest(i)
        return push(E3.at[i, :, :, p], RU.at[q, :, :, p], zu_sem, (q * PIECES + k % PIECES,), to_z(z + 1))

    def z_down(k):
        i, p = k // PIECES, cols(k)
        q = dest(i)
        return push(E3.at[i, :, :, p], RD.at[q, :, :, p], zd_sem, (q * PIECES + k % PIECES,), to_z(z - 1))

    to_core.wait_recv()
    B[CHIP] = B[OWN] + B[CORE]
    chip_x.start()
    chip_y.start()
    own_scale = TOP / bound(CHIP)

    def stage1(k):
        i, p = k // PIECES, cols(k)
        swap(k).wait_recv()

        def pair(yy, xx, h):
            return L[i, yy, c, xx, h, :, p].astype(F32) + swapped[i, yy, xx, h, :, p].astype(F32)

        for yy in range(2):
            EA[i, yy, :, p] = encode(pair(yy, 1 - x, 0), own_scale)
        first_a(k).start()
        for xx in range(2):
            EB[i, xx, :, p] = encode(pair(1 - y, xx, 1), own_scale)
        first_b(k).start()
        for j in range(2):
            S[i, j, x, 0, :, p] = pair(j, x, 0)
            S[i, y, j, 1, :, p] = pair(y, j, 1)

    @pl.loop(0, TRAIL[0])
    def _(step):
        stage1(step)

    chip_x.wait_recv()
    B[PAIR] = B[CHIP] + B[FROM_X]
    pair_y.start()
    chip_y.wait_recv()
    x_back, y_back = bound(FROM_X) / TOP, bound(FROM_Y) / TOP
    pair_y.wait_recv()
    B[PLANE] = B[PAIR] + B[PAIR_Y]
    plane_bound = bound(PLANE)
    plane_scale, plane_back = TOP / plane_bound, plane_bound / TOP

    hop = 1 if Z <= 4 else Z
    up_lag, down_lag = jnp.minimum(below, hop), jnp.minimum(above, hop)

    @pl.loop(TRAIL[0], C + TRAIL[1] + max(0, min(hop, Z - 1) - PIECES))
    def _(step):
        @pl.when(step < C)
        def _():
            stage1(step)

        @pl.when(step < C + TRAIL[0])
        def _():
            k = step - TRAIL[0]
            i, p = k // PIECES, cols(k)
            first_a(k).wait_recv()
            E2[i, 0, :, p] = encode(S[i, 1 - y, x, 0, :, p] + decode(RA[i, 1 - y, :, p], x_back), plane_scale)
            second_a(k).start()
            first_b(k).wait_recv()
            E2[i, 1, :, p] = encode(S[i, y, 1 - x, 1, :, p] + decode(RB[i, 1 - x, :, p], y_back), plane_scale)
            second_b(k).start()
            S[i, y, x, 0, :, p] = S[i, y, x, 0, :, p] + decode(RA[i, y, :, p], x_back)
            S[i, y, x, 1, :, p] = S[i, y, x, 1, :, p] + decode(RB[i, x, :, p], y_back)

        @pl.when(step == TRAIL[0] + below)
        def _():
            @pl.when(below > 0)
            def _():
                row_up.wait_recv()

            B[UP] = B[PLANE] + B[BELOW]

            @pl.when(above > 0)
            def _():
                row_up.start()

        @pl.when(step == TRAIL[0] + above)
        def _():
            @pl.when(above > 0)
            def _():
                row_down.wait_recv()

            B[DOWN] = B[PLANE] + B[ABOVE]

            @pl.when(below > 0)
            def _():
                row_down.start()

        @pl.when((step >= TRAIL[1]) & (step < C + TRAIL[1]))
        def _():
            k = step - TRAIL[1]
            i, p = k // PIECES, cols(k)
            second_a(k).wait_recv()
            second_b(k).wait_recv()
            S[i, y, x, :, :, p] = S[i, y, x, :, :, p] + decode(R2[i, :, :, p], plane_back)

        def relay(lag, side, arrow, received, came, sent):
            k = jnp.clip(step - TRAIL[1] - lag, 0, C - PIECES - 1)
            i, p = k // PIECES, cols(k)
            q = dest(i)

            @pl.when((k == step - TRAIL[1] - lag) & ((q > z) if arrow is z_up else (q < z)))
            def _():
                scale = TOP / bound(sent)

                @pl.when(side > 0)
                def _():
                    arrow(k).wait_recv()
                    value = S[i, y, x, :, :, p] + decode(received[q, :, :, p], bound(came) / TOP)
                    E3[i, :, :, p] = encode(value, scale)

                @pl.when(side == 0)
                def _():
                    E3[i, :, :, p] = encode(S[i, y, x, :, :, p], scale)

                arrow(k).start()

        relay(up_lag, below, z_up, RU, BELOW, UP)
        relay(down_lag, above, z_down, RD, ABOVE, DOWN)

    def last(arrow, received, came):
        @pl.loop(C - PIECES, C)
        def _(k):
            p = cols(k)
            arrow(k).wait_recv()
            S[Z - 1, y, x, :, :, p] = S[Z - 1, y, x, :, :, p] + decode(received[z, :, :, p], bound(came) / TOP)

    @pl.when(below > 0)
    def _():
        last(z_up, RU, BELOW)

    @pl.when(above > 0)
    def _():
        last(z_down, RD, ABOVE)

    total = S[Z - 1, y, x]
    V[c, x] = total
    lanes = jnp.sum((total * total).reshape(-1, total.shape[-1]), axis=0, keepdims=True)
    N[z, y, x, c] = sum(lanes[:, i : i + 128] for i in range(0, total.shape[-1], 128))

    @pl.loop(1, n)
    def _(k):
        to_peer(N, n_sem, n - k).start()

    v_x = push(V.at[c, x], V.at[c, x], v_sem, (0,), to_x)
    v_c = push(V.at[c, x], V.at[c, x], v_sem, (1,), to_c)
    v_xc = push(V.at[c, 1 - x], V.at[c, 1 - x], v_sem, (2,), to_c)
    got_x = push(V.at[c, 1 - x], V.at[c, 1 - x], v_sem, (0,), to_x)
    got_c = push(V.at[1 - c, x], V.at[1 - c, x], v_sem, (1,), to_c)
    got_xc = push(V.at[1 - c, 1 - x], V.at[1 - c, 1 - x], v_sem, (2,), to_c)
    v_x.start()
    v_c.start()

    for copy in states:
        copy.wait()

    @pl.loop(1, n)
    def _(k):
        from_peer(N, n_sem, k).wait_recv()

    factor = clip_factor(jnp.sum(N[...]), entries)

    def update(cc, xx, p):
        at = (cc, xx, slice(None), slice(None), p)
        new_master, new_first, new_second = adam_update(factor * V[at], M[at], F[at], Q[at])
        M[at] = new_master
        F[at] = new_first
        Q[at] = new_second
        W[(z, y) + at] = new_master.astype(jnp.bfloat16)

    every = slice(None)

    def source(b):
        return nth(b // W_PIECES)

    def lift(s, b):
        block = W.at[s, y, c, x, :, :, w_cols(b)]
        return push(block, block, gu_sem, (s * W_PIECES + b % W_PIECES,), to_z(z + 1))

    def drop(s, b):
        block = W.at[s, y, c, x, :, :, w_cols(b)]
        return push(block, block, gd_sem, (s * W_PIECES + b % W_PIECES,), to_z(z - 1))

    def same(ref, sems, b, device):
        return push(ref, ref, sems, (b,), device)

    def own_a(b, yy):
        return same(W.at[z, yy, c, x, :, :, w_cols(b)], ga_sem, b, to_y)

    def own_h(b, xx):
        return same(W.at[z, 1 - y, c, xx, :, :, w_cols(b)], ha_sem, b, to_x)

    def own_c(b, cc):
        return same(W.at[z, 1 - y, cc, :, :, :, w_cols(b)], gc_sem, b, to_c)

    def ga(b, yy):
        return same(W.at[source(b), yy, c, x, 0, :, w_cols(b)], ga_sem, b, to_y)

    def gb(b, xx):
        return same(W.at[source(b), y, c, xx, 1, :, w_cols(b)], gb_sem, b, to_x)

    def ha(b, xx):
        return same(W.at[source(b), :, c, xx, 0, :, w_cols(b)], ha_sem, b, to_x)

    def hb(b, yy):
        return same(W.at[source(b), yy, c, :, 1, :, w_cols(b)], hb_sem, b, to_y)

    def gc(b, cc):
        return same(W.at[source(b), :, cc, :, :, :, w_cols(b)], gc_sem, b, to_c)

    @pl.loop(0, W_PIECES)
    def _(b):
        update(c, x, w_cols(b))
        own_a(b, y).start()

        @pl.when(above > 0)
        def _():
            lift(z, b).start()

        @pl.when(below > 0)
        def _():
            drop(z, b).start()

    got_x.wait_recv()
    v_xc.start()
    update(c, 1 - x, every)
    got_c.wait_recv()
    update(1 - c, x, every)

    @pl.loop(0, W_PIECES)
    def _(b):
        own_a(b, 1 - y).wait_recv()
        own_h(b, x).start()

    @pl.loop(W_PIECES, G + W_TRAIL[1])
    def _(step):
        @pl.when((step >= W_PIECES + W_TRAIL[0]) & (step < G + W_TRAIL[0]))
        def _():
            b = step - W_TRAIL[0]
            ga(b, 1 - y).wait_recv()
            ha(b, x).start()
            gb(b, 1 - x).wait_recv()
            hb(b, y).start()

        @pl.when(step < G)
        def _():
            b = step
            far = b // W_PIECES

            @pl.when(far <= below)
            def _():
                lift(z - far, b).wait_recv()

                @pl.when(above > 0)
                def _():
                    lift(z - far, b).start()

            @pl.when(far <= above)
            def _():
                drop(z + far, b).wait_recv()

                @pl.when(below > 0)
                def _():
                    drop(z + far, b).start()

            ga(b, y).start()
            gb(b, x).start()

        @pl.when(step == W_PIECES)
        def _():
            got_xc.wait_recv()
            update(1 - c, 1 - x, every)

            @pl.loop(0, W_PIECES)
            def _(b):
                own_h(b, 1 - x).wait_recv()
                own_c(b, c).start()

        @pl.when(step >= W_PIECES + W_TRAIL[1])
        def _():
            b = step - W_TRAIL[1]
            ha(b, 1 - x).wait_recv()
            hb(b, 1 - y).wait_recv()
            gc(b, c).start()

    @pl.loop(0, W_PIECES)
    def _(b):
        own_c(b, 1 - c).wait_recv()

    @pl.loop(W_PIECES, G)
    def _(b):
        gc(b, 1 - c).wait_recv()

    v_x.wait_send()
    v_c.wait_send()
    v_xc.wait_send()

    for copy in (to_core, chip_x, chip_y, pair_y):
        copy.wait_send()

    @pl.loop(1, n)
    def _(k):
        to_peer(N, n_sem, k).wait_send()

    @pl.loop(0, C)
    def _(k):
        swap(k).wait_send()
        first_a(k).wait_send()
        first_b(k).wait_send()
        second_a(k).wait_send()
        second_b(k).wait_send()

    @pl.loop(0, C - PIECES)
    def _(k):
        @pl.when(dest(k // PIECES) > z)
        def _():
            z_up(k).wait_send()

        @pl.when(dest(k // PIECES) < z)
        def _():
            z_down(k).wait_send()

    @pl.when(above > 0)
    def _():
        row_up.wait_send()

    @pl.when(below > 0)
    def _():
        row_down.wait_send()

    @pl.loop(0, W_PIECES)
    def _(b):
        @pl.loop(0, Z)
        def _(s):
            @pl.when((s <= z) & (above > 0))
            def _():
                lift(s, b).wait_send()

            @pl.when((s >= z) & (below > 0))
            def _():
                drop(s, b).wait_send()

    @pl.loop(0, W_PIECES)
    def _(b):
        own_a(b, y).wait_send()
        own_h(b, x).wait_send()
        own_c(b, c).wait_send()

    @pl.loop(W_PIECES, G)
    def _(b):
        ga(b, y).wait_send()
        gb(b, x).wait_send()
        ha(b, x).wait_send()
        hb(b, y).wait_send()
        gc(b, c).wait_send()


def write_out(*refs):
    srcs, dsts, sems = refs[:4], refs[4:8], refs[8]
    copies = [pltpu.make_async_copy(a, b, sems.at[i]) for i, (a, b) in enumerate(zip(srcs, dsts))]
    for copy in copies:
        copy.start()
    for copy in copies:
        copy.wait()


def body(D, R, grads, master, first_moment, second_moment):
    rows, cols = grads.shape[1:]
    Z, n = D // 2, D * R
    t = rows // (D * R * 2)
    hbm = pl.BlockSpec(memory_space=pltpu.HBM)
    vmem = pl.BlockSpec(memory_space=pltpu.VMEM)
    bf16 = jnp.bfloat16
    part = (2, 2, 2, t, cols)
    dma = pltpu.SemaphoreType.DMA
    shapes = [((Z, 2) + part, bf16)] + [(part, F32)] * 3
    held_bytes = sum(math.prod(dims) * jnp.dtype(kind).itemsize for dims, kind in shapes)
    held = pl.pallas_call(
        functools.partial(kernel, Z, R, rows * cols),
        out_shape=[pltpu.VMEM(*shape) for shape in shapes],
        in_specs=[hbm] * 4,
        out_specs=[vmem] * 4,
        scratch_shapes=[
            pltpu.VMEM((Z, 2) + part, bf16),
            pltpu.VMEM((Z,) + part, bf16),
            pltpu.VMEM((Z,) + part, F32),
            pltpu.VMEM((Z, 2, t, cols), bf16),
            pltpu.VMEM((Z, 2, t, cols), bf16),
            pltpu.VMEM((Z, 2, t, cols), bf16),
            pltpu.VMEM((Z, 2, t, cols), bf16),
            pltpu.VMEM((Z, 2, t, cols), bf16),
            pltpu.VMEM((Z, 2, t, cols), bf16),
            pltpu.VMEM((Z, 2, t, cols), bf16),
            pltpu.VMEM((Z, 2, t, cols), bf16),
            pltpu.VMEM((Z, 2, t, cols), bf16),
            pltpu.VMEM(part, F32),
            pltpu.VMEM((Z, 2, 2, 2, 1, 128), F32),
            pltpu.VMEM((12, 1, 128), F32),
            dma((PIECES * Z,)), dma((3,)),
            dma((2, PIECES * Z)), dma((2, PIECES * Z)), dma((2, PIECES * Z)),
            dma((2, PIECES * Z)), dma((2, PIECES * Z)), dma((2, PIECES * Z)), dma((2, PIECES * Z)),
            dma((2, n)), dma((2, 12)), dma((2, 3)),
            dma((2, W_PIECES * Z)), dma((2, W_PIECES * Z)), dma((2, W_PIECES * Z)),
            dma((2, W_PIECES * Z)), dma((2, W_PIECES * Z)), dma((2, W_PIECES * Z)), dma((2, W_PIECES * Z)),
        ],
        compiler_params=pltpu.CompilerParams(
            collective_id=0, has_side_effects=True, vmem_limit_bytes=VMEM_BYTES - held_bytes
        ),
    )(
        grads.reshape((Z, 2) + part),
        master.reshape(part), first_moment.reshape(part), second_moment.reshape(part),
    )
    outs = pl.pallas_call(
        write_out,
        out_shape=[jax.ShapeDtypeStruct(*shape) for shape in shapes],
        in_specs=[vmem] * 4,
        out_specs=[hbm] * 4,
        scratch_shapes=[dma((4,))],
        compiler_params=pltpu.CompilerParams(vmem_limit_bytes=1024 * 1024),
    )(*held)
    weights, new_master, new_first, new_second = outs
    block = (rows // D, cols)
    return (weights.reshape(rows, cols), new_master.reshape(block), new_first.reshape(block), new_second.reshape(block))


def solution(mesh):
    D, R = mesh.shape["dp"], mesh.shape["rep"]
    assert R == 4 and D % 2 == 0
    in_specs = (P(("dp", "rep"), None, None), P("dp", None), P("dp", None), P("dp", None))
    out_specs = (P(), P("dp", None), P("dp", None), P("dp", None))
    return jax.shard_map(
        functools.partial(body, D, R), mesh=mesh, in_specs=in_specs, out_specs=out_specs, check_vma=False
    )
```

```python
import functools
import math

import jax
import jax.numpy as jnp
from jax import lax
from jax.experimental import pallas as pl
from jax.experimental.pallas import tpu as pltpu
from jax.sharding import PartitionSpec as P

STEP = 20
MESH = pl.DeviceIdType.MESH
F32 = jnp.float32
PIECES, TRAIL = 2, (2, 4)
W_PIECES, W_TRAIL = 2, (2, 3)
VMEM_BYTES = 63 * 1024 * 1024
TOP = 2.0**14
OWN, CORE, CHIP, FROM_X, FROM_Y, ALONG_X, ALONG_Y, FAR_X, FAR_Y, PLANES = range(10)


def adam_update(clipped, master, first_moment, second_moment):
    new_first = 0.9 * first_moment + 0.1 * clipped
    new_second = 0.95 * second_moment + 0.05 * clipped * clipped
    first_hat = new_first / (1.0 - 0.9**STEP)
    second_hat = new_second / (1.0 - 0.95**STEP)
    update = first_hat / (jnp.sqrt(second_hat) + 1e-08)
    new_master = master - 0.01 * (update + 0.1 * master)
    return (new_master, new_first, new_second)


def clip_factor(squares, entries):
    threshold = 4.0 * math.sqrt(entries)
    return jnp.minimum(1.0, threshold / (jnp.sqrt(squares) + 1e-06))


def encode(value, scale):
    u = value * scale
    u2 = u * u
    u4 = u2 * u2
    return (u4 * u4 * u).astype(jnp.bfloat16)


def decode(coded, scale):
    w = coded.astype(F32)
    size = jnp.exp(jnp.log(jnp.abs(w)) * (1.0 / 9.0)) * scale
    return jnp.where(w < 0, -size, size)


def kernel(
    Z, R, entries,
    g, m_in, f_in, s_in,
    W, M, F, Q,
    L, swapped, S, EA, EB, E2, E3, RA, RB, R2, R3, V, N, B,
    load_sem, state_sem,
    g_sem, a1_sem, b1_sem, a2_sem, b2_sem, z_sem, n_sem, m_sem, p_sem, t_sem, v_sem,
    gz_sem, ga_sem, gb_sem, ha_sem, hb_sem, gc_sem,
):
    D = 2 * Z
    n = D * R
    d, r = lax.axis_index("dp"), lax.axis_index("rep")
    z, y = d // 2, d % 2
    x, c = r // 2, r % 2
    C, G = PIECES * Z, W_PIECES * Z
    to_x = (d, (1 - x) * 2 + c)
    to_y = (z * 2 + 1 - y, r)
    to_c = (d, x * 2 + 1 - c)

    def to_z(other):
        return (other * 2 + y, r)

    def push(src, dst, sems, index, device):
        return pltpu.make_async_remote_copy(
            src_ref=src, dst_ref=dst, send_sem=sems.at[(0,) + index], recv_sem=sems.at[(1,) + index],
            device_id=device, device_id_type=MESH,
        )

    def peer(k, sign):
        zz = (z + Z + sign * (k // 8)) % Z
        return zz, (y + k // 4) % 2, (x + k // 2) % 2, (c + k) % 2

    def to_peer(ref, sems, k):
        zz, yy, xx, cc = peer(k, 1)
        return push(ref.at[z, y, x, c], ref.at[z, y, x, c], sems, (k,), (zz * 2 + yy, xx * 2 + cc))

    def from_peer(ref, sems, k):
        zz, yy, xx, cc = peer(k, -1)
        return push(ref.at[zz, yy, xx, cc], ref.at[zz, yy, xx, cc], sems, (k,), (zz * 2 + yy, xx * 2 + cc))

    below, above = z, Z - 1 - z

    def dest(k):
        return (z + 1 + k) % Z

    def cols(q):
        width = g.shape[-1] // PIECES
        return pl.ds(pl.multiple_of((q % PIECES) * width, width), width)

    def w_cols(q):
        width = g.shape[-1] // W_PIECES
        return pl.ds(pl.multiple_of((q % W_PIECES) * width, width), width)

    B[...] = jnp.zeros(B.shape, F32)
    barrier = pltpu.get_barrier_semaphore()

    for device in (to_c, to_x, to_y):
        pl.semaphore_signal(barrier, inc=1, device_id=device, device_id_type=MESH)

    @pl.when(below > 0)
    def _():
        pl.semaphore_signal(barrier, inc=1, device_id=to_z(z - 1), device_id_type=MESH)

    @pl.when(above > 0)
    def _():
        pl.semaphore_signal(barrier, inc=1, device_id=to_z(z + 1), device_id_type=MESH)

    def load(k):
        return pltpu.make_async_copy(
            g.at[dest(k // PIECES), :, :, :, :, :, cols(k)], L.at[k // PIECES, :, :, :, :, :, cols(k)], load_sem.at[k]
        )

    @pl.loop(0, C)
    def _(k):
        load(k).start()

    states = [
        pltpu.make_async_copy(a, b, state_sem.at[i])
        for i, (a, b) in enumerate([(m_in, M), (f_in, F), (s_in, Q)])
    ]
    for copy in states:
        copy.start()

    @pl.loop(0, C)
    def _(k):
        load(k).wait()
        size = jnp.abs(L[k // PIECES, :, :, :, :, :, cols(k)].astype(F32))
        lanes = jnp.max(size.reshape(-1, size.shape[-1]), axis=0, keepdims=True)
        best = B[OWN]
        for i in range(0, size.shape[-1], 128):
            best = jnp.maximum(best, lanes[:, i : i + 128])
        B[OWN] = best

    pl.semaphore_wait(barrier, 3 + jnp.minimum(below, 1) + jnp.minimum(above, 1))

    def row(source, target, device):
        return push(B.at[source], B.at[target], m_sem, (target,), device)

    to_core = row(OWN, CORE, to_c)
    chip_x, chip_y = row(CHIP, FROM_X, to_x), row(CHIP, FROM_Y, to_y)
    far_x, far_y = row(ALONG_X, FAR_X, to_y), row(ALONG_Y, FAR_Y, to_x)

    def plane(k, source):
        return push(B.at[PLANES + source], B.at[PLANES + source], p_sem, (k,), to_z(dest(k)))

    to_core.start()

    def chain(j):
        @pl.when(below == j)
        def _():
            @pl.when(below > 0)
            def _():
                pl.semaphore_wait(t_sem.at[0], 1)

            @pl.when(above > 0)
            def _():
                pl.semaphore_signal(t_sem.at[0], inc=1, device_id=to_z(z + 1), device_id_type=MESH)

        @pl.when(above == j)
        def _():
            @pl.when(above > 0)
            def _():
                pl.semaphore_wait(t_sem.at[1], 1)

            @pl.when(below > 0)
            def _():
                pl.semaphore_signal(t_sem.at[1], inc=1, device_id=to_z(z - 1), device_id_type=MESH)

    chain(0)

    def swap(k):
        return push(
            L.at[k // PIECES, :, 1 - c, :, :, :, cols(k)], swapped.at[k // PIECES, :, :, :, :, cols(k)],
            g_sem, (k,), to_c,
        )

    @pl.loop(0, C)
    def _(k):
        swap(k).start()

    def bound(index):
        return jnp.maximum(jnp.max(B[index]), 1e-30)

    def first_a(k):
        i, p = k // PIECES, cols(k)
        return push(EA.at[i, :, :, p], RA.at[i, :, :, p], a1_sem, (k,), to_x)

    def first_b(k):
        i, p = k // PIECES, cols(k)
        return push(EB.at[i, :, :, p], RB.at[i, :, :, p], b1_sem, (k,), to_y)

    def second_a(k):
        i, p = k // PIECES, cols(k)
        return push(E2.at[i, 0, :, p], R2.at[i, 0, :, p], a2_sem, (k,), to_y)

    def second_b(k):
        i, p = k // PIECES, cols(k)
        return push(E2.at[i, 1, :, p], R2.at[i, 1, :, p], b2_sem, (k,), to_x)

    def along_z(k):
        i, p = k // PIECES, cols(k)
        return push(E3.at[i, :, :, p], R3.at[i, :, :, p], z_sem, (k,), to_z(dest(i)))

    to_core.wait_recv()
    B[CHIP] = B[OWN] + B[CORE]
    chip_x.start()
    chip_y.start()
    own_scale = TOP / bound(CHIP)

    def stage1(k):
        i, p = k // PIECES, cols(k)
        swap(k).wait_recv()

        def pair(yy, xx, h):
            return L[i, yy, c, xx, h, :, p].astype(F32) + swapped[i, yy, xx, h, :, p].astype(F32)

        for yy in range(2):
            EA[i, yy, :, p] = encode(pair(yy, 1 - x, 0), own_scale)
        first_a(k).start()
        for xx in range(2):
            EB[i, xx, :, p] = encode(pair(1 - y, xx, 1), own_scale)
        first_b(k).start()
        for j in range(2):
            S[i, j, x, 0, :, p] = pair(j, x, 0)
            S[i, y, j, 1, :, p] = pair(y, j, 1)

    @pl.loop(0, TRAIL[0])
    def _(step):
        stage1(step)

    chip_x.wait_recv()
    B[ALONG_X] = B[CHIP] + B[FROM_X]
    far_x.start()
    chip_y.wait_recv()
    B[ALONG_Y] = B[CHIP] + B[FROM_Y]
    far_y.start()
    x_back, y_back = bound(FROM_X) / TOP, bound(FROM_Y) / TOP
    x_scale, y_scale = TOP / bound(ALONG_X), TOP / bound(ALONG_Y)
    chain(1)

    def stage2(k):
        i, p = k // PIECES, cols(k)
        first_a(k).wait_recv()
        E2[i, 0, :, p] = encode(S[i, 1 - y, x, 0, :, p] + decode(RA[i, 1 - y, :, p], x_back), x_scale)
        second_a(k).start()
        first_b(k).wait_recv()
        E2[i, 1, :, p] = encode(S[i, y, 1 - x, 1, :, p] + decode(RB[i, 1 - x, :, p], y_back), y_scale)
        second_b(k).start()
        S[i, y, x, 0, :, p] = S[i, y, x, 0, :, p] + decode(RA[i, y, :, p], x_back)
        S[i, y, x, 1, :, p] = S[i, y, x, 1, :, p] + decode(RB[i, x, :, p], y_back)

    @pl.loop(TRAIL[0], TRAIL[1])
    def _(step):
        stage1(step)
        stage2(step - TRAIL[0])

    @pl.loop(2, Z)
    def _(j):
        chain(j)

    far_x.wait_recv()
    far_y.wait_recv()
    B[PLANES + z] = B[ALONG_X] + B[FAR_X]
    plane_scale = TOP / bound(PLANES + z)
    far_x_back, far_y_back = bound(FAR_X) / TOP, bound(FAR_Y) / TOP

    @pl.loop(0, Z - 1)
    def _(k):
        plane(k, z).start()

    @pl.loop(TRAIL[1], C + TRAIL[1])
    def _(step):
        @pl.when(step < C)
        def _():
            stage1(step)

        @pl.when(step < C + TRAIL[0])
        def _():
            stage2(step - TRAIL[0])

        k = step - TRAIL[1]
        i, p = k // PIECES, cols(k)
        second_a(k).wait_recv()
        second_b(k).wait_recv()
        both_a = S[i, y, x, 0, :, p] + decode(R2[i, 0, :, p], far_x_back)
        both_b = S[i, y, x, 1, :, p] + decode(R2[i, 1, :, p], far_y_back)

        @pl.when(k < C - PIECES)
        def _():
            E3[i, 0, :, p] = encode(both_a, plane_scale)
            E3[i, 1, :, p] = encode(both_b, plane_scale)
            along_z(k).start()

        @pl.when(k >= C - PIECES)
        def _():
            S[i, y, x, 0, :, p] = both_a
            S[i, y, x, 1, :, p] = both_b

    @pl.loop(0, Z - 1)
    def _(i):
        source = (z + Z - 1 - i) % Z
        plane(i, source).wait_recv()
        back = bound(PLANES + source) / TOP

        @pl.loop(0, PIECES)
        def _(j):
            p = cols(j)
            along_z(i * PIECES + j).wait_recv()
            S[Z - 1, y, x, :, :, p] = S[Z - 1, y, x, :, :, p] + decode(R3[i, :, :, p], back)

    total = S[Z - 1, y, x]
    V[c, x] = total
    lanes = jnp.sum((total * total).reshape(-1, total.shape[-1]), axis=0, keepdims=True)
    N[z, y, x, c] = sum(lanes[:, i : i + 128] for i in range(0, total.shape[-1], 128))

    @pl.loop(1, n)
    def _(k):
        to_peer(N, n_sem, n - k).start()

    v_x = push(V.at[c, x], V.at[c, x], v_sem, (0,), to_x)
    v_c = push(V.at[c, x], V.at[c, x], v_sem, (1,), to_c)
    v_xc = push(V.at[c, 1 - x], V.at[c, 1 - x], v_sem, (2,), to_c)
    got_x = push(V.at[c, 1 - x], V.at[c, 1 - x], v_sem, (0,), to_x)
    got_c = push(V.at[1 - c, x], V.at[1 - c, x], v_sem, (1,), to_c)
    got_xc = push(V.at[1 - c, 1 - x], V.at[1 - c, 1 - x], v_sem, (2,), to_c)
    v_x.start()
    v_c.start()

    for copy in states:
        copy.wait()

    @pl.loop(1, n)
    def _(k):
        from_peer(N, n_sem, k).wait_recv()

    factor = clip_factor(jnp.sum(N[...]), entries)

    def update(cc, xx, p):
        at = (cc, xx, slice(None), slice(None), p)
        new_master, new_first, new_second = adam_update(factor * V[at], M[at], F[at], Q[at])
        M[at] = new_master
        F[at] = new_first
        Q[at] = new_second
        W[(z, y) + at] = new_master.astype(jnp.bfloat16)

    every = slice(None)

    def source(b):
        return (z + Z - b // W_PIECES) % Z

    def gather_z(j):
        block = W.at[z, y, c, x, :, :, w_cols(j)]
        return push(block, block, gz_sem, (j,), to_z(dest(j // W_PIECES)))

    def got_z(j):
        block = W.at[source(j + W_PIECES), y, c, x, :, :, w_cols(j)]
        return push(block, block, gz_sem, (j,), to_z(dest(j // W_PIECES)))

    def same(ref, sems, b, device):
        return push(ref, ref, sems, (b,), device)

    def own_a(b, yy):
        return same(W.at[z, yy, c, x, :, :, w_cols(b)], ga_sem, b, to_y)

    def own_h(b, xx):
        return same(W.at[z, 1 - y, c, xx, :, :, w_cols(b)], ha_sem, b, to_x)

    def own_c(b, cc):
        return same(W.at[z, 1 - y, cc, :, :, :, w_cols(b)], gc_sem, b, to_c)

    def ga(b, yy):
        return same(W.at[source(b), yy, c, x, 0, :, w_cols(b)], ga_sem, b, to_y)

    def gb(b, xx):
        return same(W.at[source(b), y, c, xx, 1, :, w_cols(b)], gb_sem, b, to_x)

    def ha(b, xx):
        return same(W.at[source(b), :, c, xx, 0, :, w_cols(b)], ha_sem, b, to_x)

    def hb(b, yy):
        return same(W.at[source(b), yy, c, :, 1, :, w_cols(b)], hb_sem, b, to_y)

    def gc(b, cc):
        return same(W.at[source(b), :, cc, :, :, :, w_cols(b)], gc_sem, b, to_c)

    @pl.loop(0, W_PIECES)
    def _(b):
        update(c, x, w_cols(b))
        own_a(b, y).start()
        gather_z(b).start()

    @pl.loop(W_PIECES, G - W_PIECES)
    def _(j):
        gather_z(j).start()

    got_x.wait_recv()
    v_xc.start()
    update(c, 1 - x, every)
    got_c.wait_recv()
    update(1 - c, x, every)

    @pl.loop(0, W_PIECES)
    def _(b):
        own_a(b, 1 - y).wait_recv()
        own_h(b, x).start()

    @pl.loop(W_PIECES, G + W_TRAIL[1])
    def _(step):
        @pl.when((step >= W_PIECES + W_TRAIL[0]) & (step < G + W_TRAIL[0]))
        def _():
            b = step - W_TRAIL[0]
            ga(b, 1 - y).wait_recv()
            ha(b, x).start()
            gb(b, 1 - x).wait_recv()
            hb(b, y).start()

        @pl.when(step < G)
        def _():
            b = step
            got_z(b - W_PIECES).wait_recv()
            ga(b, y).start()
            gb(b, x).start()

        @pl.when(step == W_PIECES)
        def _():
            got_xc.wait_recv()
            update(1 - c, 1 - x, every)

            @pl.loop(0, W_PIECES)
            def _(b):
                own_h(b, 1 - x).wait_recv()
                own_c(b, c).start()

        @pl.when(step >= W_PIECES + W_TRAIL[1])
        def _():
            b = step - W_TRAIL[1]
            ha(b, 1 - x).wait_recv()
            hb(b, 1 - y).wait_recv()
            gc(b, c).start()

    @pl.loop(0, W_PIECES)
    def _(b):
        own_c(b, 1 - c).wait_recv()

    @pl.loop(W_PIECES, G)
    def _(b):
        gc(b, 1 - c).wait_recv()

    v_x.wait_send()
    v_c.wait_send()
    v_xc.wait_send()

    for copy in (to_core, chip_x, chip_y, far_x, far_y):
        copy.wait_send()

    @pl.loop(0, Z - 1)
    def _(k):
        plane(k, z).wait_send()

    @pl.loop(1, n)
    def _(k):
        to_peer(N, n_sem, k).wait_send()

    @pl.loop(0, C)
    def _(k):
        swap(k).wait_send()
        first_a(k).wait_send()
        first_b(k).wait_send()
        second_a(k).wait_send()
        second_b(k).wait_send()

    @pl.loop(0, C - PIECES)
    def _(k):
        along_z(k).wait_send()

    @pl.loop(0, G - W_PIECES)
    def _(j):
        gather_z(j).wait_send()

    @pl.loop(0, W_PIECES)
    def _(b):
        own_a(b, y).wait_send()
        own_h(b, x).wait_send()
        own_c(b, c).wait_send()

    @pl.loop(W_PIECES, G)
    def _(b):
        ga(b, y).wait_send()
        gb(b, x).wait_send()
        ha(b, x).wait_send()
        hb(b, y).wait_send()
        gc(b, c).wait_send()


def write_out(*refs):
    srcs, dsts, sems = refs[:4], refs[4:8], refs[8]
    copies = [pltpu.make_async_copy(a, b, sems.at[i]) for i, (a, b) in enumerate(zip(srcs, dsts))]
    for copy in copies:
        copy.start()
    for copy in copies:
        copy.wait()


def body(D, R, grads, master, first_moment, second_moment):
    rows, cols = grads.shape[1:]
    Z, n = D // 2, D * R
    t = rows // (D * R * 2)
    hbm = pl.BlockSpec(memory_space=pltpu.HBM)
    vmem = pl.BlockSpec(memory_space=pltpu.VMEM)
    bf16 = jnp.bfloat16
    part = (2, 2, 2, t, cols)
    dma = pltpu.SemaphoreType.DMA
    shapes = [((Z, 2) + part, bf16)] + [(part, F32)] * 3
    held_bytes = sum(math.prod(dims) * jnp.dtype(kind).itemsize for dims, kind in shapes)
    held = pl.pallas_call(
        functools.partial(kernel, Z, R, rows * cols),
        out_shape=[pltpu.VMEM(*shape) for shape in shapes],
        in_specs=[hbm] * 4,
        out_specs=[vmem] * 4,
        scratch_shapes=[
            pltpu.VMEM((Z, 2) + part, bf16),
            pltpu.VMEM((Z,) + part, bf16),
            pltpu.VMEM((Z,) + part, F32),
            pltpu.VMEM((Z, 2, t, cols), bf16),
            pltpu.VMEM((Z, 2, t, cols), bf16),
            pltpu.VMEM((Z, 2, t, cols), bf16),
            pltpu.VMEM((Z, 2, t, cols), bf16),
            pltpu.VMEM((Z, 2, t, cols), bf16),
            pltpu.VMEM((Z, 2, t, cols), bf16),
            pltpu.VMEM((Z, 2, t, cols), bf16),
            pltpu.VMEM((Z, 2, t, cols), bf16),
            pltpu.VMEM(part, F32),
            pltpu.VMEM((Z, 2, 2, 2, 1, 128), F32),
            pltpu.VMEM((PLANES + Z, 1, 128), F32),
            dma((PIECES * Z,)), dma((3,)),
            dma((2, PIECES * Z)), dma((2, PIECES * Z)), dma((2, PIECES * Z)),
            dma((2, PIECES * Z)), dma((2, PIECES * Z)), dma((2, PIECES * Z)),
            dma((2, n)), dma((2, PLANES)), dma((2, Z)), pltpu.SemaphoreType.REGULAR((2,)), dma((2, 3)),
            dma((2, W_PIECES * Z)), dma((2, W_PIECES * Z)), dma((2, W_PIECES * Z)),
            dma((2, W_PIECES * Z)), dma((2, W_PIECES * Z)), dma((2, W_PIECES * Z)),
        ],
        compiler_params=pltpu.CompilerParams(
            collective_id=0, has_side_effects=True, vmem_limit_bytes=VMEM_BYTES - held_bytes
        ),
    )(
        grads.reshape((Z, 2) + part),
        master.reshape(part), first_moment.reshape(part), second_moment.reshape(part),
    )
    outs = pl.pallas_call(
        write_out,
        out_shape=[jax.ShapeDtypeStruct(*shape) for shape in shapes],
        in_specs=[vmem] * 4,
        out_specs=[hbm] * 4,
        scratch_shapes=[dma((4,))],
        compiler_params=pltpu.CompilerParams(vmem_limit_bytes=1024 * 1024),
    )(*held)
    weights, new_master, new_first, new_second = outs
    block = (rows // D, cols)
    return (weights.reshape(rows, cols), new_master.reshape(block), new_first.reshape(block), new_second.reshape(block))


def solution(mesh):
    D, R = mesh.shape["dp"], mesh.shape["rep"]
    assert R == 4 and D % 2 == 0
    in_specs = (P(("dp", "rep"), None, None), P("dp", None), P("dp", None), P("dp", None))
    out_specs = (P(), P("dp", None), P("dp", None), P("dp", None))
    return jax.shard_map(
        functools.partial(body, D, R), mesh=mesh, in_specs=in_specs, out_specs=out_specs, check_vma=False
    )
```

```python
import functools
import math

import jax
import jax.numpy as jnp
from jax import lax
from jax.experimental import pallas as pl
from jax.experimental.pallas import tpu as pltpu
from jax.sharding import PartitionSpec as P

STEP = 20
MESH = pl.DeviceIdType.MESH
F32 = jnp.float32
PIECES, TRAIL = 2, (2, 4)
W_PIECES, W_TRAIL = 2, (2, 4)
VMEM_BYTES = 63 * 1024 * 1024
TOP = 2.0**14
OWN, CORE, CHIP, FROM_X, FROM_Y, ALONG_X, ALONG_Y, FAR_X, FAR_Y, PLANES = range(10)


def adam_update(clipped, master, first_moment, second_moment):
    new_first = 0.9 * first_moment + 0.1 * clipped
    new_second = 0.95 * second_moment + 0.05 * clipped * clipped
    first_hat = new_first / (1.0 - 0.9**STEP)
    second_hat = new_second / (1.0 - 0.95**STEP)
    update = first_hat / (jnp.sqrt(second_hat) + 1e-08)
    new_master = master - 0.01 * (update + 0.1 * master)
    return (new_master, new_first, new_second)


def clip_factor(squares, entries):
    threshold = 4.0 * math.sqrt(entries)
    return jnp.minimum(1.0, threshold / (jnp.sqrt(squares) + 1e-06))


def encode(value, scale):
    u = value * scale
    u2 = u * u
    u4 = u2 * u2
    return (u4 * u4 * u).astype(jnp.bfloat16)


def decode(coded, scale):
    w = coded.astype(F32)
    size = jnp.exp(jnp.log(jnp.abs(w)) * (1.0 / 9.0)) * scale
    return jnp.where(w < 0, -size, size)


def kernel(
    Z, R, entries,
    g, m_in, f_in, s_in,
    W, M, F, Q,
    L, swapped, S, EA, EB, E2, E3, RA, RB, R2, R3, V, N, B,
    load_sem, state_sem,
    g_sem, a1_sem, b1_sem, a2_sem, b2_sem, z_sem, n_sem, m_sem, p_sem, t_sem, v_sem,
    gz_sem, ga_sem, gb_sem, ha_sem, hb_sem, gc_sem,
):
    D = 2 * Z
    n = D * R
    d, r = lax.axis_index("dp"), lax.axis_index("rep")
    z, y = d // 2, d % 2
    x, c = r // 2, r % 2
    t = g.shape[-2]
    pieces, w_pieces = (count if t % (8 * count) == 0 else 1 for count in (PIECES, W_PIECES))
    C, G = pieces * Z, w_pieces * Z
    to_x = (d, (1 - x) * 2 + c)
    to_y = (z * 2 + 1 - y, r)
    to_c = (d, x * 2 + 1 - c)

    def to_z(other):
        return (other * 2 + y, r)

    def push(src, dst, sems, index, device):
        return pltpu.make_async_remote_copy(
            src_ref=src, dst_ref=dst, send_sem=sems.at[(0,) + index], recv_sem=sems.at[(1,) + index],
            device_id=device, device_id_type=MESH,
        )

    def peer(k, sign):
        zz = (z + Z + sign * (k // 8)) % Z
        return zz, (y + k // 4) % 2, (x + k // 2) % 2, (c + k) % 2

    def to_peer(ref, sems, k):
        zz, yy, xx, cc = peer(k, 1)
        return push(ref.at[z, y, x, c], ref.at[z, y, x, c], sems, (k,), (zz * 2 + yy, xx * 2 + cc))

    def from_peer(ref, sems, k):
        zz, yy, xx, cc = peer(k, -1)
        return push(ref.at[zz, yy, xx, cc], ref.at[zz, yy, xx, cc], sems, (k,), (zz * 2 + yy, xx * 2 + cc))

    below, above = z, Z - 1 - z

    def dest(k):
        return (z + 1 + k) % Z

    def rows(q):
        return pl.ds(pl.multiple_of((q % pieces) * (t // pieces), t // pieces), t // pieces)

    def w_rows(q):
        return pl.ds(pl.multiple_of((q % w_pieces) * (t // w_pieces), t // w_pieces), t // w_pieces)

    B[...] = jnp.zeros(B.shape, F32)
    barrier = pltpu.get_barrier_semaphore()

    for device in (to_c, to_x, to_y):
        pl.semaphore_signal(barrier, inc=1, device_id=device, device_id_type=MESH)

    @pl.when(below > 0)
    def _():
        pl.semaphore_signal(barrier, inc=1, device_id=to_z(z - 1), device_id_type=MESH)

    @pl.when(above > 0)
    def _():
        pl.semaphore_signal(barrier, inc=1, device_id=to_z(z + 1), device_id_type=MESH)

    def load(k):
        return pltpu.make_async_copy(
            g.at[dest(k // pieces), :, :, :, :, rows(k)], L.at[k // pieces, :, :, :, :, rows(k)], load_sem.at[k]
        )

    @pl.loop(0, C)
    def _(k):
        load(k).start()

    states = [
        pltpu.make_async_copy(a, b, state_sem.at[i])
        for i, (a, b) in enumerate([(m_in, M), (f_in, F), (s_in, Q)])
    ]
    for copy in states:
        copy.start()

    @pl.loop(0, C)
    def _(k):
        load(k).wait()
        size = jnp.abs(L[k // pieces, :, :, :, :, rows(k)].astype(F32))
        lanes = jnp.max(size.reshape(-1, size.shape[-1]), axis=0, keepdims=True)
        best = B[OWN]
        for i in range(0, size.shape[-1], 128):
            best = jnp.maximum(best, lanes[:, i : i + 128])
        B[OWN] = best

    pl.semaphore_wait(barrier, 3 + jnp.minimum(below, 1) + jnp.minimum(above, 1))

    def row(source, target, device):
        return push(B.at[source], B.at[target], m_sem, (target,), device)

    to_core = row(OWN, CORE, to_c)
    chip_x, chip_y = row(CHIP, FROM_X, to_x), row(CHIP, FROM_Y, to_y)
    far_x, far_y = row(ALONG_X, FAR_X, to_y), row(ALONG_Y, FAR_Y, to_x)

    def plane(k, source):
        return push(B.at[PLANES + source], B.at[PLANES + source], p_sem, (k,), to_z(dest(k)))

    to_core.start()

    def chain(j):
        @pl.when(below == j)
        def _():
            @pl.when(below > 0)
            def _():
                pl.semaphore_wait(t_sem.at[0], 1)

            @pl.when(above > 0)
            def _():
                pl.semaphore_signal(t_sem.at[0], inc=1, device_id=to_z(z + 1), device_id_type=MESH)

        @pl.when(above == j)
        def _():
            @pl.when(above > 0)
            def _():
                pl.semaphore_wait(t_sem.at[1], 1)

            @pl.when(below > 0)
            def _():
                pl.semaphore_signal(t_sem.at[1], inc=1, device_id=to_z(z - 1), device_id_type=MESH)

    chain(0)

    def swap(k):
        return push(
            L.at[k // pieces, :, 1 - c, :, :, rows(k)], swapped.at[k // pieces, :, :, :, rows(k)],
            g_sem, (k,), to_c,
        )

    @pl.loop(0, C)
    def _(k):
        swap(k).start()

    def bound(index):
        return jnp.maximum(jnp.max(B[index]), 1e-30)

    def first_a(k):
        i, p = k // pieces, rows(k)
        return push(EA.at[i, :, p], RA.at[i, :, p], a1_sem, (k,), to_x)

    def first_b(k):
        i, p = k // pieces, rows(k)
        return push(EB.at[i, :, p], RB.at[i, :, p], b1_sem, (k,), to_y)

    def second_a(k):
        i, p = k // pieces, rows(k)
        return push(E2.at[i, 0, p], R2.at[i, 0, p], a2_sem, (k,), to_y)

    def second_b(k):
        i, p = k // pieces, rows(k)
        return push(E2.at[i, 1, p], R2.at[i, 1, p], b2_sem, (k,), to_x)

    def along_z(k):
        i, p = k // pieces, rows(k)
        return push(E3.at[i, :, p], R3.at[i, :, p], z_sem, (k,), to_z(dest(i)))

    to_core.wait_recv()
    B[CHIP] = B[OWN] + B[CORE]
    chip_x.start()
    chip_y.start()
    own_scale = TOP / bound(CHIP)

    def stage1(k):
        i, p = k // pieces, rows(k)
        swap(k).wait_recv()

        def pair(yy, xx, h):
            return L[i, yy, c, xx, h, p].astype(F32) + swapped[i, yy, xx, h, p].astype(F32)

        for yy in range(2):
            EA[i, yy, p] = encode(pair(yy, 1 - x, 0), own_scale)
        first_a(k).start()
        for xx in range(2):
            EB[i, xx, p] = encode(pair(1 - y, xx, 1), own_scale)
        first_b(k).start()
        for j in range(2):
            S[i, j, x, 0, p] = pair(j, x, 0)
            S[i, y, j, 1, p] = pair(y, j, 1)

    @pl.loop(0, TRAIL[0])
    def _(step):
        stage1(step)

    chip_x.wait_recv()
    B[ALONG_X] = B[CHIP] + B[FROM_X]
    far_x.start()
    chip_y.wait_recv()
    B[ALONG_Y] = B[CHIP] + B[FROM_Y]
    far_y.start()
    x_back, y_back = bound(FROM_X) / TOP, bound(FROM_Y) / TOP
    x_scale, y_scale = TOP / bound(ALONG_X), TOP / bound(ALONG_Y)
    chain(1)

    def stage2(k):
        i, p = k // pieces, rows(k)
        first_a(k).wait_recv()
        E2[i, 0, p] = encode(S[i, 1 - y, x, 0, p] + decode(RA[i, 1 - y, p], x_back), x_scale)
        second_a(k).start()
        first_b(k).wait_recv()
        E2[i, 1, p] = encode(S[i, y, 1 - x, 1, p] + decode(RB[i, 1 - x, p], y_back), y_scale)
        second_b(k).start()
        S[i, y, x, 0, p] = S[i, y, x, 0, p] + decode(RA[i, y, p], x_back)
        S[i, y, x, 1, p] = S[i, y, x, 1, p] + decode(RB[i, x, p], y_back)

    @pl.loop(TRAIL[0], TRAIL[1])
    def _(step):
        stage1(step)
        stage2(step - TRAIL[0])

    @pl.loop(2, Z)
    def _(j):
        chain(j)

    far_x.wait_recv()
    far_y.wait_recv()
    B[PLANES + z] = B[ALONG_X] + B[FAR_X]
    plane_scale = TOP / bound(PLANES + z)
    far_x_back, far_y_back = bound(FAR_X) / TOP, bound(FAR_Y) / TOP

    @pl.loop(0, Z - 1)
    def _(k):
        plane(k, z).start()

    @pl.loop(TRAIL[1], C + TRAIL[1])
    def _(step):
        @pl.when(step < C)
        def _():
            stage1(step)

        @pl.when(step < C + TRAIL[0])
        def _():
            stage2(step - TRAIL[0])

        k = step - TRAIL[1]
        i, p = k // pieces, rows(k)
        second_a(k).wait_recv()
        second_b(k).wait_recv()
        both_a = S[i, y, x, 0, p] + decode(R2[i, 0, p], far_x_back)
        both_b = S[i, y, x, 1, p] + decode(R2[i, 1, p], far_y_back)

        @pl.when(k < C - pieces)
        def _():
            E3[i, 0, p] = encode(both_a, plane_scale)
            E3[i, 1, p] = encode(both_b, plane_scale)
            along_z(k).start()

        @pl.when(k >= C - pieces)
        def _():
            S[i, y, x, 0, p] = both_a
            S[i, y, x, 1, p] = both_b

    @pl.loop(0, Z - 1)
    def _(i):
        source = (z + Z - 1 - i) % Z
        plane(i, source).wait_recv()
        back = bound(PLANES + source) / TOP

        @pl.loop(0, pieces)
        def _(j):
            p = rows(j)
            along_z(i * pieces + j).wait_recv()
            S[Z - 1, y, x, :, p] = S[Z - 1, y, x, :, p] + decode(R3[i, :, p], back)

    total = S[Z - 1, y, x]
    V[c, x] = total
    lanes = jnp.sum((total * total).reshape(-1, total.shape[-1]), axis=0, keepdims=True)
    N[z, y, x, c] = sum(lanes[:, i : i + 128] for i in range(0, total.shape[-1], 128))

    if n <= 32:
        for k in range(n - 1, 0, -1):
            to_peer(N, n_sem, k).start()
    else:
        @pl.loop(1, n)
        def _(k):
            to_peer(N, n_sem, n - k).start()

    v_x = push(V.at[c, x], V.at[c, x], v_sem, (0,), to_x)
    v_c = push(V.at[c, x], V.at[c, x], v_sem, (1,), to_c)
    v_xc = push(V.at[c, 1 - x], V.at[c, 1 - x], v_sem, (2,), to_c)
    got_x = push(V.at[c, 1 - x], V.at[c, 1 - x], v_sem, (0,), to_x)
    got_c = push(V.at[1 - c, x], V.at[1 - c, x], v_sem, (1,), to_c)
    got_xc = push(V.at[1 - c, 1 - x], V.at[1 - c, 1 - x], v_sem, (2,), to_c)
    v_x.start()
    v_c.start()

    for copy in states:
        copy.wait()

    @pl.loop(1, n)
    def _(k):
        from_peer(N, n_sem, k).wait_recv()

    factor = clip_factor(jnp.sum(N[...]), entries)

    def update(cc, xx, p):
        at = (cc, xx, slice(None), p)
        new_master, new_first, new_second = adam_update(factor * V[at], M[at], F[at], Q[at])
        M[at] = new_master
        F[at] = new_first
        Q[at] = new_second
        W[(z, y) + at] = new_master.astype(jnp.bfloat16)

    every = slice(None)

    def source(b):
        return (z + Z - b // w_pieces) % Z

    def gather_z(j):
        block = W.at[z, y, c, x, :, w_rows(j)]
        return push(block, block, gz_sem, (j,), to_z(dest(j // w_pieces)))

    def got_z(j):
        block = W.at[source(j + w_pieces), y, c, x, :, w_rows(j)]
        return push(block, block, gz_sem, (j,), to_z(dest(j // w_pieces)))

    def same(ref, sems, b, device):
        return push(ref, ref, sems, (b,), device)

    def own_a(b, yy):
        return same(W.at[z, yy, c, x, :, w_rows(b)], ga_sem, b, to_y)

    def own_b(b, yy):
        return same(W.at[z, yy, c, 1 - x, :, w_rows(b)], hb_sem, b, to_y)

    def own_c(b, cc):
        return same(W.at[z, 1 - y, cc, :, :, w_rows(b)], gc_sem, b, to_c)

    def ga(b, yy):
        return same(W.at[source(b), yy, c, x, 0, w_rows(b)], ga_sem, b, to_y)

    def gb(b, xx):
        return same(W.at[source(b), y, c, xx, 1, w_rows(b)], gb_sem, b, to_x)

    def ha(b, xx):
        return same(W.at[source(b), :, c, xx, 0, w_rows(b)], ha_sem, b, to_x)

    def hb(b, yy):
        return same(W.at[source(b), yy, c, :, 1, w_rows(b)], hb_sem, b, to_y)

    def gc(b, cc):
        return same(W.at[source(b), :, cc, :, :, w_rows(b)], gc_sem, b, to_c)

    @pl.loop(0, w_pieces)
    def _(b):
        update(c, x, w_rows(b))
        own_a(b, y).start()
        gather_z(b).start()

    @pl.loop(w_pieces, G - w_pieces)
    def _(j):
        gather_z(j).start()

    got_x.wait_recv()
    v_xc.start()
    update(c, 1 - x, every)

    @pl.loop(0, w_pieces)
    def _(b):
        own_b(b, y).start()

    got_c.wait_recv()
    update(1 - c, x, every)

    @pl.loop(w_pieces, G + W_TRAIL[1])
    def _(step):
        @pl.when(step < G)
        def _():
            b = step
            got_z(b - w_pieces).wait_recv()
            ga(b, y).start()
            gb(b, x).start()

        @pl.when((step >= w_pieces + W_TRAIL[0]) & (step < G + W_TRAIL[0]))
        def _():
            b = step - W_TRAIL[0]
            ga(b, 1 - y).wait_recv()
            ha(b, x).start()
            gb(b, 1 - x).wait_recv()
            hb(b, y).start()

        @pl.when(step == w_pieces + 1)
        def _():
            got_xc.wait_recv()
            update(1 - c, 1 - x, every)

            @pl.loop(0, w_pieces)
            def _(b):
                own_a(b, 1 - y).wait_recv()
                own_b(b, 1 - y).wait_recv()
                own_c(b, c).start()

        @pl.when(step >= w_pieces + W_TRAIL[1])
        def _():
            b = step - W_TRAIL[1]
            ha(b, 1 - x).wait_recv()
            hb(b, 1 - y).wait_recv()
            gc(b, c).start()

    @pl.loop(0, w_pieces)
    def _(b):
        own_c(b, 1 - c).wait_recv()

    @pl.loop(w_pieces, G)
    def _(b):
        gc(b, 1 - c).wait_recv()

    v_x.wait_send()
    v_c.wait_send()
    v_xc.wait_send()

    for copy in (to_core, chip_x, chip_y, far_x, far_y):
        copy.wait_send()

    @pl.loop(0, Z - 1)
    def _(k):
        plane(k, z).wait_send()

    @pl.loop(1, n)
    def _(k):
        to_peer(N, n_sem, k).wait_send()

    @pl.loop(0, C)
    def _(k):
        swap(k).wait_send()
        first_a(k).wait_send()
        first_b(k).wait_send()
        second_a(k).wait_send()
        second_b(k).wait_send()

    @pl.loop(0, C - pieces)
    def _(k):
        along_z(k).wait_send()

    @pl.loop(0, G - w_pieces)
    def _(j):
        gather_z(j).wait_send()

    @pl.loop(0, w_pieces)
    def _(b):
        own_a(b, y).wait_send()
        own_b(b, y).wait_send()
        own_c(b, c).wait_send()

    @pl.loop(w_pieces, G)
    def _(b):
        ga(b, y).wait_send()
        gb(b, x).wait_send()
        ha(b, x).wait_send()
        hb(b, y).wait_send()
        gc(b, c).wait_send()


def write_out(*refs):
    srcs, dsts, sems = refs[:4], refs[4:8], refs[8]
    copies = [pltpu.make_async_copy(a, b, sems.at[i]) for i, (a, b) in enumerate(zip(srcs, dsts))]
    for copy in copies:
        copy.start()
    for copy in copies:
        copy.wait()


def body(D, R, grads, master, first_moment, second_moment):
    rows, cols = grads.shape[1:]
    Z, n = D // 2, D * R
    t = rows // (D * R * 2)
    hbm = pl.BlockSpec(memory_space=pltpu.HBM)
    vmem = pl.BlockSpec(memory_space=pltpu.VMEM)
    bf16 = jnp.bfloat16
    part = (2, 2, 2, t, cols)
    dma = pltpu.SemaphoreType.DMA
    shapes = [((Z, 2) + part, bf16)] + [(part, F32)] * 3
    held_bytes = sum(math.prod(dims) * jnp.dtype(kind).itemsize for dims, kind in shapes)
    held = pl.pallas_call(
        functools.partial(kernel, Z, R, rows * cols),
        out_shape=[pltpu.VMEM(*shape) for shape in shapes],
        in_specs=[hbm] * 4,
        out_specs=[vmem] * 4,
        scratch_shapes=[
            pltpu.VMEM((Z, 2) + part, bf16),
            pltpu.VMEM((Z,) + part, bf16),
            pltpu.VMEM((Z,) + part, F32),
            pltpu.VMEM((Z, 2, t, cols), bf16),
            pltpu.VMEM((Z, 2, t, cols), bf16),
            pltpu.VMEM((Z, 2, t, cols), bf16),
            pltpu.VMEM((Z, 2, t, cols), bf16),
            pltpu.VMEM((Z, 2, t, cols), bf16),
            pltpu.VMEM((Z, 2, t, cols), bf16),
            pltpu.VMEM((Z, 2, t, cols), bf16),
            pltpu.VMEM((Z, 2, t, cols), bf16),
            pltpu.VMEM(part, F32),
            pltpu.VMEM((Z, 2, 2, 2, 1, 128), F32),
            pltpu.VMEM((PLANES + Z, 1, 128), F32),
            dma((PIECES * Z,)), dma((3,)),
            dma((2, PIECES * Z)), dma((2, PIECES * Z)), dma((2, PIECES * Z)),
            dma((2, PIECES * Z)), dma((2, PIECES * Z)), dma((2, PIECES * Z)),
            dma((2, n)), dma((2, PLANES)), dma((2, Z)), pltpu.SemaphoreType.REGULAR((2,)), dma((2, 3)),
            dma((2, W_PIECES * Z)), dma((2, W_PIECES * Z)), dma((2, W_PIECES * Z)),
            dma((2, W_PIECES * Z)), dma((2, W_PIECES * Z)), dma((2, W_PIECES * Z)),
        ],
        compiler_params=pltpu.CompilerParams(
            collective_id=0, has_side_effects=True, vmem_limit_bytes=VMEM_BYTES - held_bytes
        ),
    )(
        grads.reshape((Z, 2) + part),
        master.reshape(part), first_moment.reshape(part), second_moment.reshape(part),
    )
    outs = pl.pallas_call(
        write_out,
        out_shape=[jax.ShapeDtypeStruct(*shape) for shape in shapes],
        in_specs=[vmem] * 4,
        out_specs=[hbm] * 4,
        scratch_shapes=[dma((4,))],
        compiler_params=pltpu.CompilerParams(vmem_limit_bytes=1024 * 1024),
    )(*held)
    weights, new_master, new_first, new_second = outs
    block = (rows // D, cols)
    return (weights.reshape(rows, cols), new_master.reshape(block), new_first.reshape(block), new_second.reshape(block))


def solution(mesh):
    D, R = mesh.shape["dp"], mesh.shape["rep"]
    assert R == 4 and D % 2 == 0
    in_specs = (P(("dp", "rep"), None, None), P("dp", None), P("dp", None), P("dp", None))
    out_specs = (P(), P("dp", None), P("dp", None), P("dp", None))
    return jax.shard_map(
        functools.partial(body, D, R), mesh=mesh, in_specs=in_specs, out_specs=out_specs, check_vma=False
    )
```

```python
import functools
import math

import jax
import jax.numpy as jnp
from jax import lax
from jax.experimental import pallas as pl
from jax.experimental.pallas import tpu as pltpu
from jax.sharding import PartitionSpec as P

STEP = 20
MESH = pl.DeviceIdType.MESH
F32 = jnp.float32
PIECES, TRAIL = 2, (2, 4)
W_PIECES, W_TRAIL = 2, (2, 4)
SUM_ORDER, GATHER_ORDER = (1, 2, 0), (2, 0, 1)
VMEM_BYTES = 63 * 1024 * 1024
TOP = 2.0**14
OWN, CORE, CHIP, FROM_X, FROM_Y, ALONG_X, ALONG_Y, FAR_X, FAR_Y, PLANES = range(10)


def adam_update(clipped, master, first_moment, second_moment):
    new_first = 0.9 * first_moment + 0.1 * clipped
    new_second = 0.95 * second_moment + 0.05 * clipped * clipped
    first_hat = new_first / (1.0 - 0.9**STEP)
    second_hat = new_second / (1.0 - 0.95**STEP)
    update = first_hat / (jnp.sqrt(second_hat) + 1e-08)
    new_master = master - 0.01 * (update + 0.1 * master)
    return (new_master, new_first, new_second)


def clip_factor(squares, entries):
    threshold = 4.0 * math.sqrt(entries)
    return jnp.minimum(1.0, threshold / (jnp.sqrt(squares) + 1e-06))


def encode(value, scale):
    u = value * scale
    u2 = u * u
    u4 = u2 * u2
    return (u4 * u4 * u).astype(jnp.bfloat16)


def decode(coded, scale):
    w = coded.astype(F32)
    size = jnp.exp(jnp.log(jnp.abs(w)) * (1.0 / 9.0)) * scale
    return jnp.where(w < 0, -size, size)


def kernel(
    Z, R, entries,
    g, m_in, f_in, s_in,
    W, M, F, Q,
    L, swapped, S, EA, EB, E2, E3, RA, RB, R2, R3, V, N, B,
    load_sem, state_sem,
    g_sem, a1_sem, b1_sem, a2_sem, b2_sem, z_sem, n_sem, m_sem, p_sem, t_sem, v_sem,
    gz_sem, ga_sem, gb_sem, ha_sem, hb_sem, gc_sem,
):
    D = 2 * Z
    n = D * R
    d, r = lax.axis_index("dp"), lax.axis_index("rep")
    z, y = d // 2, d % 2
    x, c = r // 2, r % 2
    t = g.shape[-2]
    pieces, w_pieces = (count if t % (8 * count) == 0 else 1 for count in (PIECES, W_PIECES))
    C, G = pieces * Z, w_pieces * Z
    to_x = (d, (1 - x) * 2 + c)
    to_y = (z * 2 + 1 - y, r)
    to_c = (d, x * 2 + 1 - c)

    def to_z(other):
        return (other * 2 + y, r)

    def push(src, dst, sems, index, device):
        return pltpu.make_async_remote_copy(
            src_ref=src, dst_ref=dst, send_sem=sems.at[(0,) + index], recv_sem=sems.at[(1,) + index],
            device_id=device, device_id_type=MESH,
        )

    def peer(k, sign):
        zz = (z + Z + sign * (k // 8)) % Z
        return zz, (y + k // 4) % 2, (x + k // 2) % 2, (c + k) % 2

    def to_peer(ref, sems, k):
        zz, yy, xx, cc = peer(k, 1)
        return push(ref.at[z, y, x, c], ref.at[z, y, x, c], sems, (k,), (zz * 2 + yy, xx * 2 + cc))

    def from_peer(ref, sems, k):
        zz, yy, xx, cc = peer(k, -1)
        return push(ref.at[zz, yy, xx, cc], ref.at[zz, yy, xx, cc], sems, (k,), (zz * 2 + yy, xx * 2 + cc))

    below, above = z, Z - 1 - z

    def mate(i, order):
        flips = (jnp.where(z % 2 == 0, z + 1, z - 1), (z + 2) % Z, Z - 1 - z)
        first, second, third = (flips[m] for m in order)
        return jnp.where(i == 0, first, jnp.where(i == 1, second, third))

    def goes_to(i, order):
        return mate(i, order) if Z == 4 else (z + 1 + i) % Z

    def comes_from(i, order):
        return mate(i, order) if Z == 4 else (z + Z - 1 - i) % Z

    def dest(k):
        return jnp.where(k == Z - 1, z, goes_to(k, SUM_ORDER))

    def rows(q):
        return pl.ds(pl.multiple_of((q % pieces) * (t // pieces), t // pieces), t // pieces)

    def w_rows(q):
        return pl.ds(pl.multiple_of((q % w_pieces) * (t // w_pieces), t // w_pieces), t // w_pieces)

    B[...] = jnp.zeros(B.shape, F32)
    barrier = pltpu.get_barrier_semaphore()

    for device in (to_c, to_x, to_y):
        pl.semaphore_signal(barrier, inc=1, device_id=device, device_id_type=MESH)

    @pl.when(below > 0)
    def _():
        pl.semaphore_signal(barrier, inc=1, device_id=to_z(z - 1), device_id_type=MESH)

    @pl.when(above > 0)
    def _():
        pl.semaphore_signal(barrier, inc=1, device_id=to_z(z + 1), device_id_type=MESH)

    def load(k):
        return pltpu.make_async_copy(
            g.at[dest(k // pieces), :, :, :, :, rows(k)], L.at[k // pieces, :, :, :, :, rows(k)], load_sem.at[k]
        )

    @pl.loop(0, C)
    def _(k):
        load(k).start()

    states = [
        pltpu.make_async_copy(a, b, state_sem.at[i])
        for i, (a, b) in enumerate([(m_in, M), (f_in, F), (s_in, Q)])
    ]
    for copy in states:
        copy.start()

    @pl.loop(0, C)
    def _(k):
        load(k).wait()
        size = jnp.abs(L[k // pieces, :, :, :, :, rows(k)].astype(F32))
        lanes = jnp.max(size.reshape(-1, size.shape[-1]), axis=0, keepdims=True)
        best = B[OWN]
        for i in range(0, size.shape[-1], 128):
            best = jnp.maximum(best, lanes[:, i : i + 128])
        B[OWN] = best

    pl.semaphore_wait(barrier, 3 + jnp.minimum(below, 1) + jnp.minimum(above, 1))

    def row(source, target, device):
        return push(B.at[source], B.at[target], m_sem, (target,), device)

    to_core = row(OWN, CORE, to_c)
    chip_x, chip_y = row(CHIP, FROM_X, to_x), row(CHIP, FROM_Y, to_y)
    far_x, far_y = row(ALONG_X, FAR_X, to_y), row(ALONG_Y, FAR_Y, to_x)

    def plane(k, source):
        return push(B.at[PLANES + source], B.at[PLANES + source], p_sem, (k,), to_z(dest(k)))

    to_core.start()

    def chain(j):
        @pl.when(below == j)
        def _():
            @pl.when(below > 0)
            def _():
                pl.semaphore_wait(t_sem.at[0], 1)

            @pl.when(above > 0)
            def _():
                pl.semaphore_signal(t_sem.at[0], inc=1, device_id=to_z(z + 1), device_id_type=MESH)

        @pl.when(above == j)
        def _():
            @pl.when(above > 0)
            def _():
                pl.semaphore_wait(t_sem.at[1], 1)

            @pl.when(below > 0)
            def _():
                pl.semaphore_signal(t_sem.at[1], inc=1, device_id=to_z(z - 1), device_id_type=MESH)

    chain(0)

    def swap(k):
        return push(
            L.at[k // pieces, :, 1 - c, :, :, rows(k)], swapped.at[k // pieces, :, :, :, rows(k)],
            g_sem, (k,), to_c,
        )

    @pl.loop(0, C)
    def _(k):
        swap(k).start()

    def bound(index):
        return jnp.maximum(jnp.max(B[index]), 1e-30)

    def first_a(k):
        i, p = k // pieces, rows(k)
        return push(EA.at[i, :, p], RA.at[i, :, p], a1_sem, (k,), to_x)

    def first_b(k):
        i, p = k // pieces, rows(k)
        return push(EB.at[i, :, p], RB.at[i, :, p], b1_sem, (k,), to_y)

    def second_a(k):
        i, p = k // pieces, rows(k)
        return push(E2.at[i, 0, p], R2.at[i, 0, p], a2_sem, (k,), to_y)

    def second_b(k):
        i, p = k // pieces, rows(k)
        return push(E2.at[i, 1, p], R2.at[i, 1, p], b2_sem, (k,), to_x)

    def along_z(k):
        i, p = k // pieces, rows(k)
        return push(E3.at[i, :, p], R3.at[i, :, p], z_sem, (k,), to_z(dest(i)))

    to_core.wait_recv()
    B[CHIP] = B[OWN] + B[CORE]
    chip_x.start()
    chip_y.start()
    own_scale = TOP / bound(CHIP)

    def stage1(k):
        i, p = k // pieces, rows(k)
        swap(k).wait_recv()

        def pair(yy, xx, h):
            return L[i, yy, c, xx, h, p].astype(F32) + swapped[i, yy, xx, h, p].astype(F32)

        for yy in range(2):
            EA[i, yy, p] = encode(pair(yy, 1 - x, 0), own_scale)
        first_a(k).start()
        for xx in range(2):
            EB[i, xx, p] = encode(pair(1 - y, xx, 1), own_scale)
        first_b(k).start()
        for j in range(2):
            S[i, j, x, 0, p] = pair(j, x, 0)
            S[i, y, j, 1, p] = pair(y, j, 1)

    @pl.loop(0, TRAIL[0])
    def _(step):
        stage1(step)

    chip_x.wait_recv()
    B[ALONG_X] = B[CHIP] + B[FROM_X]
    far_x.start()
    chip_y.wait_recv()
    B[ALONG_Y] = B[CHIP] + B[FROM_Y]
    far_y.start()
    x_back, y_back = bound(FROM_X) / TOP, bound(FROM_Y) / TOP
    x_scale, y_scale = TOP / bound(ALONG_X), TOP / bound(ALONG_Y)
    chain(1)

    def stage2(k):
        i, p = k // pieces, rows(k)
        first_a(k).wait_recv()
        E2[i, 0, p] = encode(S[i, 1 - y, x, 0, p] + decode(RA[i, 1 - y, p], x_back), x_scale)
        second_a(k).start()
        first_b(k).wait_recv()
        E2[i, 1, p] = encode(S[i, y, 1 - x, 1, p] + decode(RB[i, 1 - x, p], y_back), y_scale)
        second_b(k).start()
        S[i, y, x, 0, p] = S[i, y, x, 0, p] + decode(RA[i, y, p], x_back)
        S[i, y, x, 1, p] = S[i, y, x, 1, p] + decode(RB[i, x, p], y_back)

    @pl.loop(TRAIL[0], TRAIL[1])
    def _(step):
        stage1(step)
        stage2(step - TRAIL[0])

    @pl.loop(2, Z)
    def _(j):
        chain(j)

    far_x.wait_recv()
    far_y.wait_recv()
    B[PLANES + z] = B[ALONG_X] + B[FAR_X]
    plane_scale = TOP / bound(PLANES + z)
    far_x_back, far_y_back = bound(FAR_X) / TOP, bound(FAR_Y) / TOP

    @pl.loop(0, Z - 1)
    def _(k):
        plane(k, z).start()

    @pl.loop(TRAIL[1], C + TRAIL[1])
    def _(step):
        @pl.when(step < C)
        def _():
            stage1(step)

        @pl.when(step < C + TRAIL[0])
        def _():
            stage2(step - TRAIL[0])

        k = step - TRAIL[1]
        i, p = k // pieces, rows(k)
        second_a(k).wait_recv()
        second_b(k).wait_recv()
        both_a = S[i, y, x, 0, p] + decode(R2[i, 0, p], far_x_back)
        both_b = S[i, y, x, 1, p] + decode(R2[i, 1, p], far_y_back)

        @pl.when(k < C - pieces)
        def _():
            E3[i, 0, p] = encode(both_a, plane_scale)
            E3[i, 1, p] = encode(both_b, plane_scale)
            along_z(k).start()

        @pl.when(k >= C - pieces)
        def _():
            S[i, y, x, 0, p] = both_a
            S[i, y, x, 1, p] = both_b

    @pl.loop(0, Z - 1)
    def _(i):
        source = comes_from(i, SUM_ORDER)
        plane(i, source).wait_recv()
        back = bound(PLANES + source) / TOP

        @pl.loop(0, pieces)
        def _(j):
            p = rows(j)
            along_z(i * pieces + j).wait_recv()
            S[Z - 1, y, x, :, p] = S[Z - 1, y, x, :, p] + decode(R3[i, :, p], back)

    total = S[Z - 1, y, x]
    V[c, x] = total
    lanes = jnp.sum((total * total).reshape(-1, total.shape[-1]), axis=0, keepdims=True)
    N[z, y, x, c] = sum(lanes[:, i : i + 128] for i in range(0, total.shape[-1], 128))

    if n <= 32:
        for k in range(n - 1, 0, -1):
            to_peer(N, n_sem, k).start()
    else:
        @pl.loop(1, n)
        def _(k):
            to_peer(N, n_sem, n - k).start()

    v_x = push(V.at[c, x], V.at[c, x], v_sem, (0,), to_x)
    v_c = push(V.at[c, x], V.at[c, x], v_sem, (1,), to_c)
    v_xc = push(V.at[c, 1 - x], V.at[c, 1 - x], v_sem, (2,), to_c)
    got_x = push(V.at[c, 1 - x], V.at[c, 1 - x], v_sem, (0,), to_x)
    got_c = push(V.at[1 - c, x], V.at[1 - c, x], v_sem, (1,), to_c)
    got_xc = push(V.at[1 - c, 1 - x], V.at[1 - c, 1 - x], v_sem, (2,), to_c)
    v_x.start()
    v_c.start()

    for copy in states:
        copy.wait()

    @pl.loop(1, n)
    def _(k):
        from_peer(N, n_sem, k).wait_recv()

    factor = clip_factor(jnp.sum(N[...]), entries)

    def update(cc, xx, p):
        at = (cc, xx, slice(None), p)
        new_master, new_first, new_second = adam_update(factor * V[at], M[at], F[at], Q[at])
        M[at] = new_master
        F[at] = new_first
        Q[at] = new_second
        W[(z, y) + at] = new_master.astype(jnp.bfloat16)

    every = slice(None)

    def source(b):
        return jnp.where(b < w_pieces, z, comes_from(b // w_pieces - 1, GATHER_ORDER))

    def gather_z(j):
        block = W.at[z, y, c, x, :, w_rows(j)]
        return push(block, block, gz_sem, (j,), to_z(goes_to(j // w_pieces, GATHER_ORDER)))

    def got_z(j):
        block = W.at[source(j + w_pieces), y, c, x, :, w_rows(j)]
        return push(block, block, gz_sem, (j,), to_z(goes_to(j // w_pieces, GATHER_ORDER)))

    def same(ref, sems, b, device):
        return push(ref, ref, sems, (b,), device)

    def own_a(b, yy):
        return same(W.at[z, yy, c, x, :, w_rows(b)], ga_sem, b, to_y)

    def own_b(b, yy):
        return same(W.at[z, yy, c, 1 - x, :, w_rows(b)], hb_sem, b, to_y)

    def own_c(b, cc):
        return same(W.at[z, 1 - y, cc, :, :, w_rows(b)], gc_sem, b, to_c)

    def ga(b, yy):
        return same(W.at[source(b), yy, c, x, 0, w_rows(b)], ga_sem, b, to_y)

    def gb(b, xx):
        return same(W.at[source(b), y, c, xx, 1, w_rows(b)], gb_sem, b, to_x)

    def ha(b, xx):
        return same(W.at[source(b), :, c, xx, 0, w_rows(b)], ha_sem, b, to_x)

    def hb(b, yy):
        return same(W.at[source(b), yy, c, :, 1, w_rows(b)], hb_sem, b, to_y)

    def gc(b, cc):
        return same(W.at[source(b), :, cc, :, :, w_rows(b)], gc_sem, b, to_c)

    @pl.loop(0, w_pieces)
    def _(b):
        update(c, x, w_rows(b))
        own_a(b, y).start()
        gather_z(b).start()

    @pl.loop(w_pieces, G - w_pieces)
    def _(j):
        gather_z(j).start()

    got_x.wait_recv()
    v_xc.start()
    update(c, 1 - x, every)

    @pl.loop(0, w_pieces)
    def _(b):
        own_b(b, y).start()

    got_c.wait_recv()
    update(1 - c, x, every)

    @pl.loop(w_pieces, G + W_TRAIL[1])
    def _(step):
        @pl.when(step < G)
        def _():
            b = step
            got_z(b - w_pieces).wait_recv()
            ga(b, y).start()
            gb(b, x).start()

        @pl.when((step >= w_pieces + W_TRAIL[0]) & (step < G + W_TRAIL[0]))
        def _():
            b = step - W_TRAIL[0]
            ga(b, 1 - y).wait_recv()
            ha(b, x).start()
            gb(b, 1 - x).wait_recv()
            hb(b, y).start()

        @pl.when(step == w_pieces + 1)
        def _():
            got_xc.wait_recv()
            update(1 - c, 1 - x, every)

            @pl.loop(0, w_pieces)
            def _(b):
                own_a(b, 1 - y).wait_recv()
                own_b(b, 1 - y).wait_recv()
                own_c(b, c).start()

        @pl.when(step >= w_pieces + W_TRAIL[1])
        def _():
            b = step - W_TRAIL[1]
            ha(b, 1 - x).wait_recv()
            hb(b, 1 - y).wait_recv()
            gc(b, c).start()

    @pl.loop(0, w_pieces)
    def _(b):
        own_c(b, 1 - c).wait_recv()

    @pl.loop(w_pieces, G)
    def _(b):
        gc(b, 1 - c).wait_recv()

    v_x.wait_send()
    v_c.wait_send()
    v_xc.wait_send()

    for copy in (to_core, chip_x, chip_y, far_x, far_y):
        copy.wait_send()

    @pl.loop(0, Z - 1)
    def _(k):
        plane(k, z).wait_send()

    @pl.loop(1, n)
    def _(k):
        to_peer(N, n_sem, k).wait_send()

    @pl.loop(0, C)
    def _(k):
        swap(k).wait_send()
        first_a(k).wait_send()
        first_b(k).wait_send()
        second_a(k).wait_send()
        second_b(k).wait_send()

    @pl.loop(0, C - pieces)
    def _(k):
        along_z(k).wait_send()

    @pl.loop(0, G - w_pieces)
    def _(j):
        gather_z(j).wait_send()

    @pl.loop(0, w_pieces)
    def _(b):
        own_a(b, y).wait_send()
        own_b(b, y).wait_send()
        own_c(b, c).wait_send()

    @pl.loop(w_pieces, G)
    def _(b):
        ga(b, y).wait_send()
        gb(b, x).wait_send()
        ha(b, x).wait_send()
        hb(b, y).wait_send()
        gc(b, c).wait_send()


def write_out(*refs):
    srcs, dsts, sems = refs[:4], refs[4:8], refs[8]
    copies = [pltpu.make_async_copy(a, b, sems.at[i]) for i, (a, b) in enumerate(zip(srcs, dsts))]
    for copy in copies:
        copy.start()
    for copy in copies:
        copy.wait()


def body(D, R, grads, master, first_moment, second_moment):
    rows, cols = grads.shape[1:]
    Z, n = D // 2, D * R
    t = rows // (D * R * 2)
    hbm = pl.BlockSpec(memory_space=pltpu.HBM)
    vmem = pl.BlockSpec(memory_space=pltpu.VMEM)
    bf16 = jnp.bfloat16
    part = (2, 2, 2, t, cols)
    dma = pltpu.SemaphoreType.DMA
    shapes = [((Z, 2) + part, bf16)] + [(part, F32)] * 3
    held_bytes = sum(math.prod(dims) * jnp.dtype(kind).itemsize for dims, kind in shapes)
    held = pl.pallas_call(
        functools.partial(kernel, Z, R, rows * cols),
        out_shape=[pltpu.VMEM(*shape) for shape in shapes],
        in_specs=[hbm] * 4,
        out_specs=[vmem] * 4,
        scratch_shapes=[
            pltpu.VMEM((Z, 2) + part, bf16),
            pltpu.VMEM((Z,) + part, bf16),
            pltpu.VMEM((Z,) + part, F32),
            pltpu.VMEM((Z, 2, t, cols), bf16),
            pltpu.VMEM((Z, 2, t, cols), bf16),
            pltpu.VMEM((Z, 2, t, cols), bf16),
            pltpu.VMEM((Z, 2, t, cols), bf16),
            pltpu.VMEM((Z, 2, t, cols), bf16),
            pltpu.VMEM((Z, 2, t, cols), bf16),
            pltpu.VMEM((Z, 2, t, cols), bf16),
            pltpu.VMEM((Z, 2, t, cols), bf16),
            pltpu.VMEM(part, F32),
            pltpu.VMEM((Z, 2, 2, 2, 1, 128), F32),
            pltpu.VMEM((PLANES + Z, 1, 128), F32),
            dma((PIECES * Z,)), dma((3,)),
            dma((2, PIECES * Z)), dma((2, PIECES * Z)), dma((2, PIECES * Z)),
            dma((2, PIECES * Z)), dma((2, PIECES * Z)), dma((2, PIECES * Z)),
            dma((2, n)), dma((2, PLANES)), dma((2, Z)), pltpu.SemaphoreType.REGULAR((2,)), dma((2, 3)),
            dma((2, W_PIECES * Z)), dma((2, W_PIECES * Z)), dma((2, W_PIECES * Z)),
            dma((2, W_PIECES * Z)), dma((2, W_PIECES * Z)), dma((2, W_PIECES * Z)),
        ],
        compiler_params=pltpu.CompilerParams(
            collective_id=0, has_side_effects=True, vmem_limit_bytes=VMEM_BYTES - held_bytes
        ),
    )(
        grads.reshape((Z, 2) + part),
        master.reshape(part), first_moment.reshape(part), second_moment.reshape(part),
    )
    outs = pl.pallas_call(
        write_out,
        out_shape=[jax.ShapeDtypeStruct(*shape) for shape in shapes],
        in_specs=[vmem] * 4,
        out_specs=[hbm] * 4,
        scratch_shapes=[dma((4,))],
        compiler_params=pltpu.CompilerParams(vmem_limit_bytes=1024 * 1024),
    )(*held)
    weights, new_master, new_first, new_second = outs
    block = (rows // D, cols)
    return (weights.reshape(rows, cols), new_master.reshape(block), new_first.reshape(block), new_second.reshape(block))


def solution(mesh):
    D, R = mesh.shape["dp"], mesh.shape["rep"]
    assert R == 4 and D % 2 == 0
    in_specs = (P(("dp", "rep"), None, None), P("dp", None), P("dp", None), P("dp", None))
    out_specs = (P(), P("dp", None), P("dp", None), P("dp", None))
    return jax.shard_map(
        functools.partial(body, D, R), mesh=mesh, in_specs=in_specs, out_specs=out_specs, check_vma=False
    )
```

```python
import functools
import math

import jax
import jax.numpy as jnp
from jax import lax
from jax.experimental import pallas as pl
from jax.experimental.pallas import tpu as pltpu
from jax.sharding import PartitionSpec as P

STEP = 20
MESH = pl.DeviceIdType.MESH
F32 = jnp.float32
PIECES, TRAIL = 2, (2, 4)
W_PIECES, W_TRAIL = 2, (2, 4)
SUM_ORDER, GATHER_ORDER = (1, 2, 0), (2, 0, 1)
VMEM_BYTES = 63 * 1024 * 1024
TOP = 2.0**14
OWN, CORE, CHIP, FROM_X, FROM_Y, ALONG_X, ALONG_Y, FAR_X, FAR_Y, PLANES = range(10)


def adam_update(clipped, master, first_moment, second_moment):
    new_first = 0.9 * first_moment + 0.1 * clipped
    new_second = 0.95 * second_moment + 0.05 * clipped * clipped
    first_hat = new_first / (1.0 - 0.9**STEP)
    second_hat = new_second / (1.0 - 0.95**STEP)
    update = first_hat / (jnp.sqrt(second_hat) + 1e-08)
    new_master = master - 0.01 * (update + 0.1 * master)
    return (new_master, new_first, new_second)


def clip_factor(squares, entries):
    threshold = 4.0 * math.sqrt(entries)
    return jnp.minimum(1.0, threshold / (jnp.sqrt(squares) + 1e-06))


def encode(value, scale):
    u = value * scale
    u2 = u * u
    u4 = u2 * u2
    return (u4 * u4 * u).astype(jnp.bfloat16)


def decode(coded, scale):
    w = coded.astype(F32)
    size = jnp.exp(jnp.log(jnp.abs(w)) * (1.0 / 9.0)) * scale
    return jnp.where(w < 0, -size, size)


def kernel(
    Z, R, entries,
    g, m_in, f_in, s_in,
    W, M, F, Q,
    L, swapped, S, EA, EB, E2, E3, RA, RB, R2, R3, V, N, B,
    load_sem, state_sem,
    g_sem, a1_sem, b1_sem, a2_sem, b2_sem, z_sem, n_sem, m_sem, p_sem, t_sem, v_sem,
    gz_sem, ga_sem, gb_sem, ha_sem, hb_sem, gc_sem,
):
    D = 2 * Z
    n = D * R
    d, r = lax.axis_index("dp"), lax.axis_index("rep")
    z, y = d // 2, d % 2
    x, c = r // 2, r % 2
    t = g.shape[-2]
    pieces, w_pieces = (count if t % (8 * count) == 0 else 1 for count in (PIECES, W_PIECES))
    C, G = pieces * Z, w_pieces * Z
    to_x = (d, (1 - x) * 2 + c)
    to_y = (z * 2 + 1 - y, r)
    to_c = (d, x * 2 + 1 - c)

    def to_z(other):
        return (other * 2 + y, r)

    def push(src, dst, sems, index, device):
        return pltpu.make_async_remote_copy(
            src_ref=src, dst_ref=dst, send_sem=sems.at[(0,) + index], recv_sem=sems.at[(1,) + index],
            device_id=device, device_id_type=MESH,
        )

    def peer(k, sign):
        zz = (z + Z + sign * (k // 8)) % Z
        return zz, (y + k // 4) % 2, (x + k // 2) % 2, (c + k) % 2

    def to_peer(ref, sems, k):
        zz, yy, xx, cc = peer(k, 1)
        return push(ref.at[z, y, x, c], ref.at[z, y, x, c], sems, (k,), (zz * 2 + yy, xx * 2 + cc))

    def from_peer(ref, sems, k):
        zz, yy, xx, cc = peer(k, -1)
        return push(ref.at[zz, yy, xx, cc], ref.at[zz, yy, xx, cc], sems, (k,), (zz * 2 + yy, xx * 2 + cc))

    below, above = z, Z - 1 - z

    def mate(i, order):
        flips = (jnp.where(z % 2 == 0, z + 1, z - 1), (z + 2) % Z, Z - 1 - z)
        first, second, third = (flips[m] for m in order)
        return jnp.where(i == 0, first, jnp.where(i == 1, second, third))

    def goes_to(i, order):
        return mate(i, order) if Z == 4 else (z + 1 + i) % Z

    def comes_from(i, order):
        return mate(i, order) if Z == 4 else (z + Z - 1 - i) % Z

    def dest(k):
        return jnp.where(k == Z - 1, z, goes_to(k, SUM_ORDER))

    def rows(q):
        return pl.ds(pl.multiple_of((q % pieces) * (t // pieces), t // pieces), t // pieces)

    def w_rows(q):
        return pl.ds(pl.multiple_of((q % w_pieces) * (t // w_pieces), t // w_pieces), t // w_pieces)

    B[...] = jnp.zeros(B.shape, F32)
    barrier = pltpu.get_barrier_semaphore()

    for device in (to_c, to_x, to_y):
        pl.semaphore_signal(barrier, inc=1, device_id=device, device_id_type=MESH)

    @pl.when(below > 0)
    def _():
        pl.semaphore_signal(barrier, inc=1, device_id=to_z(z - 1), device_id_type=MESH)

    @pl.when(above > 0)
    def _():
        pl.semaphore_signal(barrier, inc=1, device_id=to_z(z + 1), device_id_type=MESH)

    def load(k):
        return pltpu.make_async_copy(
            g.at[dest(k // pieces), :, :, :, :, rows(k)], L.at[k // pieces, :, :, :, :, rows(k)], load_sem.at[k]
        )

    @pl.loop(0, C)
    def _(k):
        load(k).start()

    states = [
        pltpu.make_async_copy(a, b, state_sem.at[i])
        for i, (a, b) in enumerate([(m_in, M), (f_in, F), (s_in, Q)])
    ]
    for copy in states:
        copy.start()

    @pl.loop(0, C)
    def _(k):
        load(k).wait()
        size = jnp.abs(L[k // pieces, :, :, :, :, rows(k)].astype(F32))
        lanes = jnp.max(size.reshape(-1, size.shape[-1]), axis=0, keepdims=True)
        best = B[OWN]
        for i in range(0, size.shape[-1], 128):
            best = jnp.maximum(best, lanes[:, i : i + 128])
        B[OWN] = best

    pl.semaphore_wait(barrier, 3 + jnp.minimum(below, 1) + jnp.minimum(above, 1))

    def row(source, target, device):
        return push(B.at[source], B.at[target], m_sem, (target,), device)

    to_core = row(OWN, CORE, to_c)
    chip_x, chip_y = row(CHIP, FROM_X, to_x), row(CHIP, FROM_Y, to_y)
    far_x, far_y = row(ALONG_X, FAR_X, to_y), row(ALONG_Y, FAR_Y, to_x)

    def plane(k, source):
        return push(B.at[PLANES + source], B.at[PLANES + source], p_sem, (k,), to_z(dest(k)))

    to_core.start()

    def chain(j):
        @pl.when(below == j)
        def _():
            @pl.when(below > 0)
            def _():
                pl.semaphore_wait(t_sem.at[0], 1)

            @pl.when(above > 0)
            def _():
                pl.semaphore_signal(t_sem.at[0], inc=1, device_id=to_z(z + 1), device_id_type=MESH)

        @pl.when(above == j)
        def _():
            @pl.when(above > 0)
            def _():
                pl.semaphore_wait(t_sem.at[1], 1)

            @pl.when(below > 0)
            def _():
                pl.semaphore_signal(t_sem.at[1], inc=1, device_id=to_z(z - 1), device_id_type=MESH)

    chain(0)

    def swap(k):
        return push(
            L.at[k // pieces, :, 1 - c, :, :, rows(k)], swapped.at[k // pieces, :, :, :, rows(k)],
            g_sem, (k,), to_c,
        )

    @pl.loop(0, C)
    def _(k):
        swap(k).start()

    def bound(index):
        return jnp.maximum(jnp.max(B[index]), 1e-30)

    def first_a(k):
        i, p = k // pieces, rows(k)
        return push(EA.at[i, :, p], RA.at[i, :, p], a1_sem, (k,), to_x)

    def first_b(k):
        i, p = k // pieces, rows(k)
        return push(EB.at[i, :, p], RB.at[i, :, p], b1_sem, (k,), to_y)

    def second_a(k):
        i, p = k // pieces, rows(k)
        return push(E2.at[i, 0, p], R2.at[i, 0, p], a2_sem, (k,), to_y)

    def second_b(k):
        i, p = k // pieces, rows(k)
        return push(E2.at[i, 1, p], R2.at[i, 1, p], b2_sem, (k,), to_x)

    def along_z(k):
        i, p = k // pieces, rows(k)
        return push(E3.at[i, :, p], R3.at[i, :, p], z_sem, (k,), to_z(dest(i)))

    to_core.wait_recv()
    B[CHIP] = B[OWN] + B[CORE]
    chip_x.start()
    chip_y.start()
    own_scale = TOP / bound(CHIP)

    def stage1(k):
        i, p = k // pieces, rows(k)
        swap(k).wait_recv()

        def pair(yy, xx, h):
            return L[i, yy, c, xx, h, p].astype(F32) + swapped[i, yy, xx, h, p].astype(F32)

        for yy in range(2):
            EA[i, yy, p] = encode(pair(yy, 1 - x, 0), own_scale)
        first_a(k).start()
        for xx in range(2):
            EB[i, xx, p] = encode(pair(1 - y, xx, 1), own_scale)
        first_b(k).start()
        for j in range(2):
            S[i, j, x, 0, p] = pair(j, x, 0)
            S[i, y, j, 1, p] = pair(y, j, 1)

    @pl.loop(0, TRAIL[0])
    def _(step):
        stage1(step)

    chip_x.wait_recv()
    B[ALONG_X] = B[CHIP] + B[FROM_X]
    far_x.start()
    chip_y.wait_recv()
    B[ALONG_Y] = B[CHIP] + B[FROM_Y]
    far_y.start()
    x_back, y_back = bound(FROM_X) / TOP, bound(FROM_Y) / TOP
    x_scale, y_scale = TOP / bound(ALONG_X), TOP / bound(ALONG_Y)
    chain(1)

    def stage2(k):
        i, p = k // pieces, rows(k)
        first_a(k).wait_recv()
        E2[i, 0, p] = encode(S[i, 1 - y, x, 0, p] + decode(RA[i, 1 - y, p], x_back), x_scale)
        second_a(k).start()
        first_b(k).wait_recv()
        E2[i, 1, p] = encode(S[i, y, 1 - x, 1, p] + decode(RB[i, 1 - x, p], y_back), y_scale)
        second_b(k).start()
        S[i, y, x, 0, p] = S[i, y, x, 0, p] + decode(RA[i, y, p], x_back)
        S[i, y, x, 1, p] = S[i, y, x, 1, p] + decode(RB[i, x, p], y_back)

    @pl.loop(TRAIL[0], TRAIL[1])
    def _(step):
        stage1(step)
        stage2(step - TRAIL[0])

    @pl.loop(2, Z)
    def _(j):
        chain(j)

    far_x.wait_recv()
    far_y.wait_recv()
    B[PLANES + z] = B[ALONG_X] + B[FAR_X]
    plane_scale = TOP / bound(PLANES + z)
    far_x_back, far_y_back = bound(FAR_X) / TOP, bound(FAR_Y) / TOP

    @pl.loop(0, Z - 1)
    def _(k):
        plane(k, z).start()

    @pl.loop(TRAIL[1], C + TRAIL[1])
    def _(step):
        @pl.when(step < C)
        def _():
            stage1(step)

        @pl.when(step < C + TRAIL[0])
        def _():
            stage2(step - TRAIL[0])

        k = step - TRAIL[1]
        i, p = k // pieces, rows(k)
        second_a(k).wait_recv()
        second_b(k).wait_recv()
        both_a = S[i, y, x, 0, p] + decode(R2[i, 0, p], far_x_back)
        both_b = S[i, y, x, 1, p] + decode(R2[i, 1, p], far_y_back)

        @pl.when(k < C - pieces)
        def _():
            E3[i, 0, p] = encode(both_a, plane_scale)
            E3[i, 1, p] = encode(both_b, plane_scale)
            along_z(k).start()

        @pl.when(k >= C - pieces)
        def _():
            S[i, y, x, 0, p] = both_a
            S[i, y, x, 1, p] = both_b

    @pl.loop(0, Z - 1)
    def _(i):
        source = comes_from(i, SUM_ORDER)
        plane(i, source).wait_recv()
        back = bound(PLANES + source) / TOP

        @pl.loop(0, pieces)
        def _(j):
            p = rows(j)
            along_z(i * pieces + j).wait_recv()
            S[Z - 1, y, x, :, p] = S[Z - 1, y, x, :, p] + decode(R3[i, :, p], back)

    total = S[Z - 1, y, x]
    V[c, x] = total
    lanes = jnp.sum((total * total).reshape(-1, total.shape[-1]), axis=0, keepdims=True)
    N[z, y, x, c] = sum(lanes[:, i : i + 128] for i in range(0, total.shape[-1], 128))

    if n <= 32:
        for k in range(n - 1, 0, -1):
            to_peer(N, n_sem, k).start()
    else:
        @pl.loop(1, n)
        def _(k):
            to_peer(N, n_sem, n - k).start()

    v_x = push(V.at[c, x], V.at[c, x], v_sem, (0,), to_x)
    v_c = push(V.at[c, x], V.at[c, x], v_sem, (1,), to_c)
    v_xc = push(V.at[c, 1 - x], V.at[c, 1 - x], v_sem, (2,), to_c)
    got_x = push(V.at[c, 1 - x], V.at[c, 1 - x], v_sem, (0,), to_x)
    got_c = push(V.at[1 - c, x], V.at[1 - c, x], v_sem, (1,), to_c)
    got_xc = push(V.at[1 - c, 1 - x], V.at[1 - c, 1 - x], v_sem, (2,), to_c)
    v_x.start()
    v_c.start()

    for copy in states:
        copy.wait()

    @pl.loop(1, n)
    def _(k):
        from_peer(N, n_sem, k).wait_recv()

    factor = clip_factor(jnp.sum(N[...]), entries)

    def update(cc, xx, p):
        at = (cc, xx, slice(None), p)
        new_master, new_first, new_second = adam_update(factor * V[at], M[at], F[at], Q[at])
        M[at] = new_master
        F[at] = new_first
        Q[at] = new_second
        W[(z, y) + at] = new_master.astype(jnp.bfloat16)

    every = slice(None)

    def source(b):
        return jnp.where(b < w_pieces, z, comes_from(b // w_pieces - 1, GATHER_ORDER))

    def gather_z(j):
        block = W.at[z, y, c, x, :, w_rows(j)]
        return push(block, block, gz_sem, (j,), to_z(goes_to(j // w_pieces, GATHER_ORDER)))

    def got_z(j):
        block = W.at[source(j + w_pieces), y, c, x, :, w_rows(j)]
        return push(block, block, gz_sem, (j,), to_z(goes_to(j // w_pieces, GATHER_ORDER)))

    def same(ref, sems, b, device):
        return push(ref, ref, sems, (b,), device)

    def own_a(b, yy):
        return same(W.at[z, yy, c, x, :, w_rows(b)], ga_sem, b, to_y)

    def own_b(b, yy):
        return same(W.at[z, yy, c, 1 - x, :, w_rows(b)], hb_sem, b, to_y)

    def own_c(b, cc):
        return same(W.at[z, 1 - y, cc, :, :, w_rows(b)], gc_sem, b, to_c)

    def ga(b, yy):
        return same(W.at[source(b), yy, c, x, 0, w_rows(b)], ga_sem, b, to_y)

    def gb(b, xx):
        return same(W.at[source(b), y, c, xx, 1, w_rows(b)], gb_sem, b, to_x)

    def ha(b, xx):
        return same(W.at[source(b), :, c, xx, 0, w_rows(b)], ha_sem, b, to_x)

    def hb(b, yy):
        return same(W.at[source(b), yy, c, :, 1, w_rows(b)], hb_sem, b, to_y)

    def gc(b, cc):
        return same(W.at[source(b), :, cc, :, :, w_rows(b)], gc_sem, b, to_c)

    @pl.loop(0, w_pieces)
    def _(b):
        update(c, x, w_rows(b))
        own_a(b, y).start()
        gather_z(b).start()

    @pl.loop(w_pieces, G - w_pieces)
    def _(j):
        gather_z(j).start()

    got_x.wait_recv()
    v_xc.start()
    update(c, 1 - x, every)

    @pl.loop(0, w_pieces)
    def _(b):
        own_b(b, y).start()

    got_c.wait_recv()
    update(1 - c, x, every)

    @pl.loop(w_pieces, G + W_TRAIL[1])
    def _(step):
        @pl.when(step < G)
        def _():
            b = step
            got_z(b - w_pieces).wait_recv()
            ga(b, y).start()
            gb(b, x).start()

        @pl.when((step >= w_pieces + W_TRAIL[0]) & (step < G + W_TRAIL[0]))
        def _():
            b = step - W_TRAIL[0]
            ga(b, 1 - y).wait_recv()
            ha(b, x).start()
            gb(b, 1 - x).wait_recv()
            hb(b, y).start()

        @pl.when(step == w_pieces + 3)
        def _():
            got_xc.wait_recv()
            update(1 - c, 1 - x, every)

            @pl.loop(0, w_pieces)
            def _(b):
                own_a(b, 1 - y).wait_recv()
                own_b(b, 1 - y).wait_recv()
                own_c(b, c).start()

        @pl.when(step >= w_pieces + W_TRAIL[1])
        def _():
            b = step - W_TRAIL[1]
            ha(b, 1 - x).wait_recv()
            hb(b, 1 - y).wait_recv()
            gc(b, c).start()

    @pl.loop(0, w_pieces)
    def _(b):
        own_c(b, 1 - c).wait_recv()

    @pl.loop(w_pieces, G)
    def _(b):
        gc(b, 1 - c).wait_recv()

    v_x.wait_send()
    v_c.wait_send()
    v_xc.wait_send()

    for copy in (to_core, chip_x, chip_y, far_x, far_y):
        copy.wait_send()

    @pl.loop(0, Z - 1)
    def _(k):
        plane(k, z).wait_send()

    @pl.loop(1, n)
    def _(k):
        to_peer(N, n_sem, k).wait_send()

    @pl.loop(0, C)
    def _(k):
        swap(k).wait_send()
        first_a(k).wait_send()
        first_b(k).wait_send()
        second_a(k).wait_send()
        second_b(k).wait_send()

    @pl.loop(0, C - pieces)
    def _(k):
        along_z(k).wait_send()

    @pl.loop(0, G - w_pieces)
    def _(j):
        gather_z(j).wait_send()

    @pl.loop(0, w_pieces)
    def _(b):
        own_a(b, y).wait_send()
        own_b(b, y).wait_send()
        own_c(b, c).wait_send()

    @pl.loop(w_pieces, G)
    def _(b):
        ga(b, y).wait_send()
        gb(b, x).wait_send()
        ha(b, x).wait_send()
        hb(b, y).wait_send()
        gc(b, c).wait_send()


def write_out(*refs):
    srcs, dsts, sems = refs[:4], refs[4:8], refs[8]
    copies = [pltpu.make_async_copy(a, b, sems.at[i]) for i, (a, b) in enumerate(zip(srcs, dsts))]
    for copy in copies:
        copy.start()
    for copy in copies:
        copy.wait()


def body(D, R, grads, master, first_moment, second_moment):
    rows, cols = grads.shape[1:]
    Z, n = D // 2, D * R
    t = rows // (D * R * 2)
    hbm = pl.BlockSpec(memory_space=pltpu.HBM)
    vmem = pl.BlockSpec(memory_space=pltpu.VMEM)
    bf16 = jnp.bfloat16
    part = (2, 2, 2, t, cols)
    dma = pltpu.SemaphoreType.DMA
    shapes = [((Z, 2) + part, bf16)] + [(part, F32)] * 3
    held_bytes = sum(math.prod(dims) * jnp.dtype(kind).itemsize for dims, kind in shapes)
    held = pl.pallas_call(
        functools.partial(kernel, Z, R, rows * cols),
        out_shape=[pltpu.VMEM(*shape) for shape in shapes],
        in_specs=[hbm] * 4,
        out_specs=[vmem] * 4,
        scratch_shapes=[
            pltpu.VMEM((Z, 2) + part, bf16),
            pltpu.VMEM((Z,) + part, bf16),
            pltpu.VMEM((Z,) + part, F32),
            pltpu.VMEM((Z, 2, t, cols), bf16),
            pltpu.VMEM((Z, 2, t, cols), bf16),
            pltpu.VMEM((Z, 2, t, cols), bf16),
            pltpu.VMEM((Z, 2, t, cols), bf16),
            pltpu.VMEM((Z, 2, t, cols), bf16),
            pltpu.VMEM((Z, 2, t, cols), bf16),
            pltpu.VMEM((Z, 2, t, cols), bf16),
            pltpu.VMEM((Z, 2, t, cols), bf16),
            pltpu.VMEM(part, F32),
            pltpu.VMEM((Z, 2, 2, 2, 1, 128), F32),
            pltpu.VMEM((PLANES + Z, 1, 128), F32),
            dma((PIECES * Z,)), dma((3,)),
            dma((2, PIECES * Z)), dma((2, PIECES * Z)), dma((2, PIECES * Z)),
            dma((2, PIECES * Z)), dma((2, PIECES * Z)), dma((2, PIECES * Z)),
            dma((2, n)), dma((2, PLANES)), dma((2, Z)), pltpu.SemaphoreType.REGULAR((2,)), dma((2, 3)),
            dma((2, W_PIECES * Z)), dma((2, W_PIECES * Z)), dma((2, W_PIECES * Z)),
            dma((2, W_PIECES * Z)), dma((2, W_PIECES * Z)), dma((2, W_PIECES * Z)),
        ],
        compiler_params=pltpu.CompilerParams(
            collective_id=0, has_side_effects=True, vmem_limit_bytes=VMEM_BYTES - held_bytes
        ),
    )(
        grads.reshape((Z, 2) + part),
        master.reshape(part), first_moment.reshape(part), second_moment.reshape(part),
    )
    outs = pl.pallas_call(
        write_out,
        out_shape=[jax.ShapeDtypeStruct(*shape) for shape in shapes],
        in_specs=[vmem] * 4,
        out_specs=[hbm] * 4,
        scratch_shapes=[dma((4,))],
        compiler_params=pltpu.CompilerParams(vmem_limit_bytes=1024 * 1024),
    )(*held)
    weights, new_master, new_first, new_second = outs
    block = (rows // D, cols)
    return (weights.reshape(rows, cols), new_master.reshape(block), new_first.reshape(block), new_second.reshape(block))


def solution(mesh):
    D, R = mesh.shape["dp"], mesh.shape["rep"]
    assert R == 4 and D % 2 == 0
    in_specs = (P(("dp", "rep"), None, None), P("dp", None), P("dp", None), P("dp", None))
    out_specs = (P(), P("dp", None), P("dp", None), P("dp", None))
    return jax.shard_map(
        functools.partial(body, D, R), mesh=mesh, in_specs=in_specs, out_specs=out_specs, check_vma=False
    )
```

```python
import functools
import math

import jax
import jax.numpy as jnp
from jax import lax
from jax.experimental import pallas as pl
from jax.experimental.pallas import tpu as pltpu
from jax.sharding import PartitionSpec as P

STEP = 20
MESH = pl.DeviceIdType.MESH
F32 = jnp.float32
PIECES, TRAIL = 2, (2, 4)
W_PIECES, W_TRAIL = 2, (2, 4)
SUM_ORDER, GATHER_ORDER = (1, 2, 0), (2, 0, 1)
VMEM_BYTES = 63 * 1024 * 1024
TOP = 2.0**14
OWN, CORE, CHIP, FROM_X, FROM_Y, ALONG_X, ALONG_Y, FAR_X, FAR_Y, PLANES = range(10)


def adam_update(clipped, master, first_moment, second_moment):
    new_first = 0.9 * first_moment + 0.1 * clipped
    new_second = 0.95 * second_moment + 0.05 * clipped * clipped
    first_hat = new_first / (1.0 - 0.9**STEP)
    second_hat = new_second / (1.0 - 0.95**STEP)
    update = first_hat / (jnp.sqrt(second_hat) + 1e-08)
    new_master = master - 0.01 * (update + 0.1 * master)
    return (new_master, new_first, new_second)


def clip_factor(squares, entries):
    threshold = 4.0 * math.sqrt(entries)
    return jnp.minimum(1.0, threshold / (jnp.sqrt(squares) + 1e-06))


def encode(value, scale):
    u = value * scale
    u2 = u * u
    u4 = u2 * u2
    return (u4 * u4 * u).astype(jnp.bfloat16)


def decode(coded, scale):
    w = coded.astype(F32)
    size = jnp.exp(jnp.log(jnp.abs(w)) * (1.0 / 9.0)) * scale
    return jnp.where(w < 0, -size, size)


def kernel(
    Z, R, entries,
    g, m_in, f_in, s_in,
    W, M, F, Q,
    L, swapped, S, EA, EB, E2, E3, RA, RB, R2, R3, V, N, B,
    load_sem, state_sem,
    g_sem, a1_sem, b1_sem, a2_sem, b2_sem, z_sem, n_sem, m_sem, p_sem, t_sem, v_sem,
    gz_sem, ga_sem, gb_sem, ha_sem, hb_sem, gc_sem,
):
    D = 2 * Z
    n = D * R
    d, r = lax.axis_index("dp"), lax.axis_index("rep")
    z, y = d // 2, d % 2
    x, c = r // 2, r % 2
    t = g.shape[-2]
    pieces, w_pieces = (count if t % (8 * count) == 0 else 1 for count in (PIECES, W_PIECES))
    C, G = pieces * Z, w_pieces * Z
    to_x = (d, (1 - x) * 2 + c)
    to_y = (z * 2 + 1 - y, r)
    to_c = (d, x * 2 + 1 - c)

    def to_z(other):
        return (other * 2 + y, r)

    def push(src, dst, sems, index, device):
        return pltpu.make_async_remote_copy(
            src_ref=src, dst_ref=dst, send_sem=sems.at[(0,) + index], recv_sem=sems.at[(1,) + index],
            device_id=device, device_id_type=MESH,
        )

    def peer(k, sign):
        zz = (z + Z + sign * (k // 8)) % Z
        return zz, (y + k // 4) % 2, (x + k // 2) % 2, (c + k) % 2

    def to_peer(ref, sems, k):
        zz, yy, xx, cc = peer(k, 1)
        return push(ref.at[z, y, x, c], ref.at[z, y, x, c], sems, (k,), (zz * 2 + yy, xx * 2 + cc))

    def from_peer(ref, sems, k):
        zz, yy, xx, cc = peer(k, -1)
        return push(ref.at[zz, yy, xx, cc], ref.at[zz, yy, xx, cc], sems, (k,), (zz * 2 + yy, xx * 2 + cc))

    below, above = z, Z - 1 - z

    def mate(i, order):
        flips = (jnp.where(z % 2 == 0, z + 1, z - 1), (z + 2) % Z, Z - 1 - z)
        first, second, third = (flips[m] for m in order)
        return jnp.where(i == 0, first, jnp.where(i == 1, second, third))

    def goes_to(i, order):
        return mate(i, order) if Z == 4 else (z + 1 + i) % Z

    def comes_from(i, order):
        return mate(i, order) if Z == 4 else (z + Z - 1 - i) % Z

    def dest(k):
        return jnp.where(k == Z - 1, z, goes_to(k, SUM_ORDER))

    def rows(q):
        return pl.ds(pl.multiple_of((q % pieces) * (t // pieces), t // pieces), t // pieces)

    def w_rows(q):
        return pl.ds(pl.multiple_of((q % w_pieces) * (t // w_pieces), t // w_pieces), t // w_pieces)

    B[...] = jnp.zeros(B.shape, F32)
    barrier = pltpu.get_barrier_semaphore()

    for device in (to_c, to_x, to_y):
        pl.semaphore_signal(barrier, inc=1, device_id=device, device_id_type=MESH)

    @pl.when(below > 0)
    def _():
        pl.semaphore_signal(barrier, inc=1, device_id=to_z(z - 1), device_id_type=MESH)

    @pl.when(above > 0)
    def _():
        pl.semaphore_signal(barrier, inc=1, device_id=to_z(z + 1), device_id_type=MESH)

    def load(k):
        return pltpu.make_async_copy(
            g.at[dest(k // pieces), :, :, :, :, rows(k)], L.at[k // pieces, :, :, :, :, rows(k)], load_sem.at[k]
        )

    @pl.loop(0, C)
    def _(k):
        load(k).start()

    states = [
        pltpu.make_async_copy(a, b, state_sem.at[i])
        for i, (a, b) in enumerate([(m_in, M), (f_in, F), (s_in, Q)])
    ]
    for copy in states:
        copy.start()

    @pl.loop(0, C)
    def _(k):
        load(k).wait()
        size = jnp.abs(L[k // pieces, :, :, :, :, rows(k)].astype(F32))
        lanes = jnp.max(size.reshape(-1, size.shape[-1]), axis=0, keepdims=True)
        best = B[OWN]
        for i in range(0, size.shape[-1], 128):
            best = jnp.maximum(best, lanes[:, i : i + 128])
        B[OWN] = best

    pl.semaphore_wait(barrier, 3 + jnp.minimum(below, 1) + jnp.minimum(above, 1))

    def row(source, target, device):
        return push(B.at[source], B.at[target], m_sem, (target,), device)

    to_core = row(OWN, CORE, to_c)
    chip_x, chip_y = row(CHIP, FROM_X, to_x), row(CHIP, FROM_Y, to_y)
    far_x, far_y = row(ALONG_X, FAR_X, to_y), row(ALONG_Y, FAR_Y, to_x)

    def plane(k, source):
        return push(B.at[PLANES + source], B.at[PLANES + source], p_sem, (k,), to_z(dest(k)))

    to_core.start()

    def chain(j):
        @pl.when(below == j)
        def _():
            @pl.when(below > 0)
            def _():
                pl.semaphore_wait(t_sem.at[0], 1)

            @pl.when(above > 0)
            def _():
                pl.semaphore_signal(t_sem.at[0], inc=1, device_id=to_z(z + 1), device_id_type=MESH)

        @pl.when(above == j)
        def _():
            @pl.when(above > 0)
            def _():
                pl.semaphore_wait(t_sem.at[1], 1)

            @pl.when(below > 0)
            def _():
                pl.semaphore_signal(t_sem.at[1], inc=1, device_id=to_z(z - 1), device_id_type=MESH)

    chain(0)

    def swap(k):
        return push(
            L.at[k // pieces, :, 1 - c, :, :, rows(k)], swapped.at[k // pieces, :, :, :, rows(k)],
            g_sem, (k,), to_c,
        )

    @pl.loop(0, C)
    def _(k):
        swap(k).start()

    def bound(index):
        return jnp.maximum(jnp.max(B[index]), 1e-30)

    def first_a(k):
        i, p = k // pieces, rows(k)
        return push(EA.at[i, :, p], RA.at[i, :, p], a1_sem, (k,), to_x)

    def first_b(k):
        i, p = k // pieces, rows(k)
        return push(EB.at[i, :, p], RB.at[i, :, p], b1_sem, (k,), to_y)

    def second_a(k):
        i, p = k // pieces, rows(k)
        return push(E2.at[i, 0, p], R2.at[i, 0, p], a2_sem, (k,), to_y)

    def second_b(k):
        i, p = k // pieces, rows(k)
        return push(E2.at[i, 1, p], R2.at[i, 1, p], b2_sem, (k,), to_x)

    def along_z(k):
        i, p = k // pieces, rows(k)
        return push(E3.at[i, :, p], R3.at[i, :, p], z_sem, (k,), to_z(dest(i)))

    to_core.wait_recv()
    B[CHIP] = B[OWN] + B[CORE]
    chip_x.start()
    chip_y.start()
    own_scale = TOP / bound(CHIP)

    def stage1(k):
        i, p = k // pieces, rows(k)
        swap(k).wait_recv()

        def pair(yy, xx, h):
            return L[i, yy, c, xx, h, p].astype(F32) + swapped[i, yy, xx, h, p].astype(F32)

        for yy in range(2):
            EA[i, yy, p] = encode(pair(yy, 1 - x, 0), own_scale)
        first_a(k).start()
        for xx in range(2):
            EB[i, xx, p] = encode(pair(1 - y, xx, 1), own_scale)
        first_b(k).start()
        for j in range(2):
            S[i, j, x, 0, p] = pair(j, x, 0)
            S[i, y, j, 1, p] = pair(y, j, 1)

    @pl.loop(0, TRAIL[0])
    def _(step):
        stage1(step)

    chip_x.wait_recv()
    B[ALONG_X] = B[CHIP] + B[FROM_X]
    far_x.start()
    chip_y.wait_recv()
    B[ALONG_Y] = B[CHIP] + B[FROM_Y]
    far_y.start()
    x_back, y_back = bound(FROM_X) / TOP, bound(FROM_Y) / TOP
    x_scale, y_scale = TOP / bound(ALONG_X), TOP / bound(ALONG_Y)
    chain(1)

    def stage2(k):
        i, p = k // pieces, rows(k)
        first_a(k).wait_recv()
        E2[i, 0, p] = encode(S[i, 1 - y, x, 0, p] + decode(RA[i, 1 - y, p], x_back), x_scale)
        second_a(k).start()
        first_b(k).wait_recv()
        E2[i, 1, p] = encode(S[i, y, 1 - x, 1, p] + decode(RB[i, 1 - x, p], y_back), y_scale)
        second_b(k).start()
        S[i, y, x, 0, p] = S[i, y, x, 0, p] + decode(RA[i, y, p], x_back)
        S[i, y, x, 1, p] = S[i, y, x, 1, p] + decode(RB[i, x, p], y_back)

    @pl.loop(TRAIL[0], TRAIL[1])
    def _(step):
        stage1(step)
        stage2(step - TRAIL[0])

    @pl.loop(2, Z)
    def _(j):
        chain(j)

    far_x.wait_recv()
    far_y.wait_recv()
    B[PLANES + z] = B[ALONG_X] + B[FAR_X]
    plane_scale = TOP / bound(PLANES + z)
    far_x_back, far_y_back = bound(FAR_X) / TOP, bound(FAR_Y) / TOP

    @pl.loop(0, Z - 1)
    def _(k):
        plane(k, z).start()

    @pl.loop(TRAIL[1], C + TRAIL[1])
    def _(step):
        @pl.when(step < C)
        def _():
            stage1(step)

        @pl.when(step < C + TRAIL[0])
        def _():
            stage2(step - TRAIL[0])

        k = step - TRAIL[1]
        i, p = k // pieces, rows(k)
        second_a(k).wait_recv()
        second_b(k).wait_recv()
        both_a = S[i, y, x, 0, p] + decode(R2[i, 0, p], far_x_back)
        both_b = S[i, y, x, 1, p] + decode(R2[i, 1, p], far_y_back)

        @pl.when(k < C - pieces)
        def _():
            E3[i, 0, p] = encode(both_a, plane_scale)
            E3[i, 1, p] = encode(both_b, plane_scale)
            along_z(k).start()

        @pl.when(k >= C - pieces)
        def _():
            S[i, y, x, 0, p] = both_a
            S[i, y, x, 1, p] = both_b

    @pl.loop(0, Z - 1)
    def _(i):
        source = comes_from(i, SUM_ORDER)
        plane(i, source).wait_recv()
        back = bound(PLANES + source) / TOP

        @pl.loop(0, pieces)
        def _(j):
            p = rows(j)
            along_z(i * pieces + j).wait_recv()
            S[Z - 1, y, x, :, p] = S[Z - 1, y, x, :, p] + decode(R3[i, :, p], back)

    total = S[Z - 1, y, x]
    V[c, x] = total
    lanes = jnp.sum((total * total).reshape(-1, total.shape[-1]), axis=0, keepdims=True)
    N[z, y, x, c] = sum(lanes[:, i : i + 128] for i in range(0, total.shape[-1], 128))

    if n <= 32:
        for k in range(n - 1, 0, -1):
            to_peer(N, n_sem, k).start()
    else:
        @pl.loop(1, n)
        def _(k):
            to_peer(N, n_sem, n - k).start()

    v_x = push(V.at[c, x], V.at[c, x], v_sem, (0,), to_x)
    v_c = push(V.at[c, x], V.at[c, x], v_sem, (1,), to_c)
    v_xc = push(V.at[c, 1 - x], V.at[c, 1 - x], v_sem, (2,), to_c)
    got_x = push(V.at[c, 1 - x], V.at[c, 1 - x], v_sem, (0,), to_x)
    got_c = push(V.at[1 - c, x], V.at[1 - c, x], v_sem, (1,), to_c)
    got_xc = push(V.at[1 - c, 1 - x], V.at[1 - c, 1 - x], v_sem, (2,), to_c)
    v_x.start()
    v_c.start()

    for copy in states:
        copy.wait()

    @pl.loop(1, n)
    def _(k):
        from_peer(N, n_sem, k).wait_recv()

    factor = clip_factor(jnp.sum(N[...]), entries)

    def update(cc, xx, p):
        at = (cc, xx, slice(None), p)
        new_master, new_first, new_second = adam_update(factor * V[at], M[at], F[at], Q[at])
        M[at] = new_master
        F[at] = new_first
        Q[at] = new_second
        W[(z, y) + at] = new_master.astype(jnp.bfloat16)

    every = slice(None)

    def source(b):
        return jnp.where(b < w_pieces, z, comes_from(b // w_pieces - 1, GATHER_ORDER))

    def gather_z(j):
        block = W.at[z, y, c, x, :, w_rows(j)]
        return push(block, block, gz_sem, (j,), to_z(goes_to(j // w_pieces, GATHER_ORDER)))

    def got_z(j):
        block = W.at[source(j + w_pieces), y, c, x, :, w_rows(j)]
        return push(block, block, gz_sem, (j,), to_z(goes_to(j // w_pieces, GATHER_ORDER)))

    def same(ref, sems, b, device):
        return push(ref, ref, sems, (b,), device)

    def own_a(b, yy):
        return same(W.at[z, yy, c, x, :, w_rows(b)], ga_sem, b, to_y)

    def own_b(b, yy):
        return same(W.at[z, yy, c, 1 - x, :, w_rows(b)], hb_sem, b, to_y)

    def own_c(b, cc):
        return same(W.at[z, 1 - y, cc, :, :, w_rows(b)], gc_sem, b, to_c)

    def ga(b, yy):
        return same(W.at[source(b), yy, c, x, 0, w_rows(b)], ga_sem, b, to_y)

    def gb(b, xx):
        return same(W.at[source(b), y, c, xx, 1, w_rows(b)], gb_sem, b, to_x)

    def ha(b, xx):
        return same(W.at[source(b), :, c, xx, 0, w_rows(b)], ha_sem, b, to_x)

    def hb(b, yy):
        return same(W.at[source(b), yy, c, :, 1, w_rows(b)], hb_sem, b, to_y)

    def gc(b, cc):
        return same(W.at[source(b), :, cc, :, :, w_rows(b)], gc_sem, b, to_c)

    @pl.loop(0, w_pieces)
    def _(b):
        update(c, x, w_rows(b))
        own_a(b, y).start()
        gather_z(b).start()

    @pl.loop(w_pieces, G - w_pieces)
    def _(j):
        gather_z(j).start()

    got_x.wait_recv()
    v_xc.start()
    update(c, 1 - x, every)

    @pl.loop(0, w_pieces)
    def _(b):
        own_b(b, y).start()

    @pl.loop(w_pieces, G + W_TRAIL[1])
    def _(step):
        @pl.when(step < G)
        def _():
            b = step
            got_z(b - w_pieces).wait_recv()
            ga(b, y).start()
            gb(b, x).start()

        @pl.when((step >= w_pieces + W_TRAIL[0]) & (step < G + W_TRAIL[0]))
        def _():
            b = step - W_TRAIL[0]
            ga(b, 1 - y).wait_recv()
            ha(b, x).start()
            gb(b, 1 - x).wait_recv()
            hb(b, y).start()

        @pl.when(step == w_pieces + 3)
        def _():
            got_c.wait_recv()
            update(1 - c, x, every)
            got_xc.wait_recv()
            update(1 - c, 1 - x, every)

            @pl.loop(0, w_pieces)
            def _(b):
                own_a(b, 1 - y).wait_recv()
                own_b(b, 1 - y).wait_recv()
                own_c(b, c).start()

        @pl.when(step >= w_pieces + W_TRAIL[1])
        def _():
            b = step - W_TRAIL[1]
            ha(b, 1 - x).wait_recv()
            hb(b, 1 - y).wait_recv()
            gc(b, c).start()

    @pl.loop(0, w_pieces)
    def _(b):
        own_c(b, 1 - c).wait_recv()

    @pl.loop(w_pieces, G)
    def _(b):
        gc(b, 1 - c).wait_recv()

    v_x.wait_send()
    v_c.wait_send()
    v_xc.wait_send()

    for copy in (to_core, chip_x, chip_y, far_x, far_y):
        copy.wait_send()

    @pl.loop(0, Z - 1)
    def _(k):
        plane(k, z).wait_send()

    @pl.loop(1, n)
    def _(k):
        to_peer(N, n_sem, k).wait_send()

    @pl.loop(0, C)
    def _(k):
        swap(k).wait_send()
        first_a(k).wait_send()
        first_b(k).wait_send()
        second_a(k).wait_send()
        second_b(k).wait_send()

    @pl.loop(0, C - pieces)
    def _(k):
        along_z(k).wait_send()

    @pl.loop(0, G - w_pieces)
    def _(j):
        gather_z(j).wait_send()

    @pl.loop(0, w_pieces)
    def _(b):
        own_a(b, y).wait_send()
        own_b(b, y).wait_send()
        own_c(b, c).wait_send()

    @pl.loop(w_pieces, G)
    def _(b):
        ga(b, y).wait_send()
        gb(b, x).wait_send()
        ha(b, x).wait_send()
        hb(b, y).wait_send()
        gc(b, c).wait_send()


def write_out(*refs):
    srcs, dsts, sems = refs[:4], refs[4:8], refs[8]
    copies = [pltpu.make_async_copy(a, b, sems.at[i]) for i, (a, b) in enumerate(zip(srcs, dsts))]
    for copy in copies:
        copy.start()
    for copy in copies:
        copy.wait()


def body(D, R, grads, master, first_moment, second_moment):
    rows, cols = grads.shape[1:]
    Z, n = D // 2, D * R
    t = rows // (D * R * 2)
    hbm = pl.BlockSpec(memory_space=pltpu.HBM)
    vmem = pl.BlockSpec(memory_space=pltpu.VMEM)
    bf16 = jnp.bfloat16
    part = (2, 2, 2, t, cols)
    dma = pltpu.SemaphoreType.DMA
    shapes = [((Z, 2) + part, bf16)] + [(part, F32)] * 3
    held_bytes = sum(math.prod(dims) * jnp.dtype(kind).itemsize for dims, kind in shapes)
    held = pl.pallas_call(
        functools.partial(kernel, Z, R, rows * cols),
        out_shape=[pltpu.VMEM(*shape) for shape in shapes],
        in_specs=[hbm] * 4,
        out_specs=[vmem] * 4,
        scratch_shapes=[
            pltpu.VMEM((Z, 2) + part, bf16),
            pltpu.VMEM((Z,) + part, bf16),
            pltpu.VMEM((Z,) + part, F32),
            pltpu.VMEM((Z, 2, t, cols), bf16),
            pltpu.VMEM((Z, 2, t, cols), bf16),
            pltpu.VMEM((Z, 2, t, cols), bf16),
            pltpu.VMEM((Z, 2, t, cols), bf16),
            pltpu.VMEM((Z, 2, t, cols), bf16),
            pltpu.VMEM((Z, 2, t, cols), bf16),
            pltpu.VMEM((Z, 2, t, cols), bf16),
            pltpu.VMEM((Z, 2, t, cols), bf16),
            pltpu.VMEM(part, F32),
            pltpu.VMEM((Z, 2, 2, 2, 1, 128), F32),
            pltpu.VMEM((PLANES + Z, 1, 128), F32),
            dma((PIECES * Z,)), dma((3,)),
            dma((2, PIECES * Z)), dma((2, PIECES * Z)), dma((2, PIECES * Z)),
            dma((2, PIECES * Z)), dma((2, PIECES * Z)), dma((2, PIECES * Z)),
            dma((2, n)), dma((2, PLANES)), dma((2, Z)), pltpu.SemaphoreType.REGULAR((2,)), dma((2, 3)),
            dma((2, W_PIECES * Z)), dma((2, W_PIECES * Z)), dma((2, W_PIECES * Z)),
            dma((2, W_PIECES * Z)), dma((2, W_PIECES * Z)), dma((2, W_PIECES * Z)),
        ],
        compiler_params=pltpu.CompilerParams(
            collective_id=0, has_side_effects=True, vmem_limit_bytes=VMEM_BYTES - held_bytes
        ),
    )(
        grads.reshape((Z, 2) + part),
        master.reshape(part), first_moment.reshape(part), second_moment.reshape(part),
    )
    outs = pl.pallas_call(
        write_out,
        out_shape=[jax.ShapeDtypeStruct(*shape) for shape in shapes],
        in_specs=[vmem] * 4,
        out_specs=[hbm] * 4,
        scratch_shapes=[dma((4,))],
        compiler_params=pltpu.CompilerParams(vmem_limit_bytes=1024 * 1024),
    )(*held)
    weights, new_master, new_first, new_second = outs
    block = (rows // D, cols)
    return (weights.reshape(rows, cols), new_master.reshape(block), new_first.reshape(block), new_second.reshape(block))


def solution(mesh):
    D, R = mesh.shape["dp"], mesh.shape["rep"]
    assert R == 4 and D % 2 == 0
    in_specs = (P(("dp", "rep"), None, None), P("dp", None), P("dp", None), P("dp", None))
    out_specs = (P(), P("dp", None), P("dp", None), P("dp", None))
    return jax.shard_map(
        functools.partial(body, D, R), mesh=mesh, in_specs=in_specs, out_specs=out_specs, check_vma=False
    )
```
